32 devices in a mesh: tok: 8 (over z, x), feat: 4 (over y, core).
Axes of the slice: x: 2, y: 2, z: 4, core: 2. Of those that a mesh axis runs over, the one named last changes fastest.
Arguments:
- queries: bfloat16 [1024, 4096], P('tok', 'feat'), may hold values from -12 to 12
- keys: bfloat16 [1024, 1024], P('tok', 'feat'), may hold values from -12 to 12
- values: bfloat16 [1024, 1024], P('tok', 'feat'), may hold values from -6 to 6
- out_weight: bfloat16 [4096, 4096], P('feat', 'tok'), may hold values from -0.09375 to 0.09375
- doc_lengths: int32 [6], replicated, may hold values from 1 to 640, 1024 in all
Outputs:
- mixed: bfloat16 [1024, 4096], P('tok', 'feat')
The draws below stay inside these ranges and needn't reach their ends.
Inputs may be any that keep to these rules, and one draw needn't show every extreme that they name: `doc_lengths`: the lengths sum to 1024, and the largest is exactly 640.
All inputs are finite; a program needn't handle non-finite values.
Results may differ from the reference program's by a relative error of at most 0.012.
The reference program's roundings to bfloat16 on the way count: a program that leaves them out, or rounds other values in their place, can miss the bound.
Values may be sent and summed in bfloat16 or wider, within the bound.
No kernel may reach another device: no remote copies, remote signals or barrier semaphores. Data moves between devices by JAX's collectives and lax.ppermute only.
A program may use at most 64 MiB of HBM per device.

```python
import math
import jax
import jax.numpy as jnp
import numpy as np
from jax import lax

QH = 32
KVH = 8
HD = 128
D = 4096
DOCS = 6
TOKENS = 1024
MOST = 640
N_FEAT = 4


def draw_queries(key, part):
    normal_part = 2.0 * jnp.clip(jax.random.normal(jax.random.fold_in(key, 1), (TOKENS, QH, HD), jnp.float32), -6.0, 6.0)
    return normal_part.reshape(TOKENS, QH * HD).astype(jnp.bfloat16)


def draw_keys(key, part):
    normal_part = 1.5 * jnp.clip(jax.random.normal(jax.random.fold_in(key, 2), (TOKENS, KVH, HD), jnp.float32), -6.0, 6.0)
    return normal_part.reshape(TOKENS, KVH * HD).astype(jnp.bfloat16)


def steps_of(own_key, extent, split, least, high):
    level = 1.0
    for position, shards_of in split:
        heights = jax.random.uniform(jax.random.fold_in(jax.random.fold_in(own_key, 6), position), (shards_of,), jnp.float32, least / len(split), high / len(split))
        level = level * jnp.repeat(jnp.exp(heights), extent[position] // shards_of).reshape((-1,) + (1,) * (len(extent) - 1 - position))
    return level


def profile(count, total, bound, lean):
    portions = [(1 << 20) // math.isqrt(grade ** lean) + 1 for grade in range(2, count + 1)]
    surplus, given = total - bound - (count - 1), [1] * (count - 1)
    while surplus > 0:
        free = [i for i in range(count - 1) if given[i] < bound]
        whole, remaining = sum([portions[i] for i in free]), surplus
        for i in free:
            more = min(bound - given[i], max(1, remaining * portions[i] // whole), surplus)
            given[i] = given[i] + more
            surplus = surplus - more
    return np.array([bound] + given)


def uneven(stream_key, number_of, total, most, skew):
    if number_of == 2:
        one = jax.random.randint(stream_key, (), max(1, total - most), min(most, total - 1) + 1)
        return jnp.stack([one, total - one])
    sizes = jnp.asarray(profile(number_of, total, most, skew), jnp.int32)
    twos = (number_of - 1) // 2
    donor, sink = sizes[1:1 + 2 * twos:2], sizes[2:2 + 2 * twos:2]
    room = jnp.minimum(donor - 1, most - sink)
    passed = jax.random.randint(jax.random.fold_in(stream_key, 1), (twos,), 0, 1 << 20) % (room + 1)
    sizes = sizes.at[1:1 + 2 * twos:2].set(donor - passed).at[2:2 + 2 * twos:2].set(sink + passed)
    return sizes[jax.random.permutation(jax.random.fold_in(stream_key, 2), number_of)]


def gaussian(key, dims, scale, most, cuts=(), held_as=jnp.bfloat16):
    entries = jax.random.normal(key, dims, jnp.float32) * scale
    if len(cuts) > 0:
        entries = steps_of(key, dims, cuts, -0.22, 0.18) * entries
    return jnp.clip(entries, min=-most, max=most).astype(held_as)


def setup_inputs(seed: int = 0) -> dict:
    key_list = jax.random.split(jax.random.key(seed), 6)
    queries = draw_queries(jax.random.fold_in(key_list[5], 71), 0)
    keys = draw_keys(jax.random.fold_in(key_list[5], 71), 0)
    values = gaussian(key_list[2], (TOKENS, KVH * HD), 1.0, 6.0, ((0, 8), (1, 4)))
    out_weight = gaussian(key_list[3], (D, D), D ** -0.5, 0.09375, ((0, 4), (1, 8)))
    doc_lengths = uneven(key_list[4], DOCS, TOKENS, MOST, 2).astype(jnp.int32)
    return dict(queries=queries, keys=keys, values=values, out_weight=out_weight, doc_lengths=doc_lengths)


ROPE_BASE = 500000.0
NEG_FILL = -1.0e30


def locate(token_index, doc_lengths):
    doc_ends = jnp.cumsum(doc_lengths).astype(jnp.int32)
    starts = doc_ends - doc_lengths
    doc_ids = jnp.sum((token_index[:, None] >= doc_ends[None, :]).astype(jnp.int32), axis=1)
    number = jnp.arange(doc_lengths.shape[0], dtype=jnp.int32)
    first_token = jnp.sum(jnp.where(doc_ids[:, None] == number[None, :], starts[None, :], 0), axis=1)
    return doc_ids, (token_index - first_token).astype(jnp.int32)


def rotary(tensor, positions):
    half_size = tensor.shape[-1] // 2
    frequency = ROPE_BASE ** (-(jnp.arange(half_size, dtype=jnp.float32) * 2.0 / tensor.shape[-1]))
    angles = positions.astype(jnp.float32)[:, None] * frequency[None, :]
    cosine = jnp.cos(angles)[:, None, :]
    sine_part = jnp.sin(angles)[:, None, :]
    first_half = tensor[..., :half_size]
    second_half = tensor[..., half_size:]
    return jnp.concatenate([first_half * cosine - second_half * sine_part, second_half * cosine + first_half * sine_part], axis=-1)


def reference(queries, keys, values, out_weight, doc_lengths):
    token_index = jnp.arange(TOKENS, dtype=jnp.int32)
    doc_ids, positions = locate(token_index, doc_lengths)
    rotated_q = rotary(queries.astype(jnp.float32).reshape(TOKENS, QH, HD), positions).astype(jnp.bfloat16)
    rotated_k = rotary(keys.astype(jnp.float32).reshape(TOKENS, KVH, HD), positions).astype(jnp.bfloat16)
    value_heads = values.reshape(TOKENS, KVH, HD)
    group_size = QH // KVH
    tile_rows = min(256, TOKENS)
    window = min(TOKENS, MOST + tile_rows)
    scale_factor = HD ** -0.5

    def one_tile(block_number):
        first_row = (block_number * tile_rows).astype(jnp.int32)
        query_tile = lax.dynamic_slice_in_dim(rotated_q, first_row, tile_rows, 0)
        query_tile = query_tile.reshape(tile_rows, KVH, group_size, HD).astype(jnp.float32)
        key_first = jnp.clip(first_row + tile_rows - window, 0, TOKENS - window).astype(jnp.int32)
        key_tile = lax.dynamic_slice_in_dim(rotated_k, key_first, window, 0).astype(jnp.float32)
        value_tile = lax.dynamic_slice_in_dim(value_heads, key_first, window, 0).astype(jnp.float32)
        scores = jnp.einsum('qgjd,kgd->gjqk', query_tile, key_tile) * scale_factor
        query_index = first_row + jnp.arange(tile_rows, dtype=jnp.int32)
        key_index = key_first + jnp.arange(window, dtype=jnp.int32)
        query_doc = lax.dynamic_slice_in_dim(doc_ids, first_row, tile_rows, 0)
        key_doc = lax.dynamic_slice_in_dim(doc_ids, key_first, window, 0)
        visible = (query_doc[:, None] == key_doc[None, :]) & (key_index[None, :] <= query_index[:, None])
        scores = jnp.where(visible, scores, NEG_FILL)
        row_max = jnp.max(scores, axis=-1, keepdims=True)
        weights = jnp.where(visible, jnp.exp(scores - row_max), 0.0)
        totals = jnp.sum(weights, axis=-1)
        rounded = lax.optimization_barrier(weights.astype(jnp.bfloat16)).astype(jnp.float32)
        output = jnp.einsum('gjqk,kgd->gjqd', rounded, value_tile) / totals[..., None]
        return output.transpose(2, 0, 1, 3).reshape(tile_rows, QH * HD).astype(jnp.bfloat16)

    attended = lax.map(one_tile, jnp.arange(TOKENS // tile_rows, dtype=jnp.int32))
    attended = attended.reshape(TOKENS, QH * HD)
    block_width = D // N_FEAT
    mixed_sum = jnp.zeros((TOKENS, D), jnp.float32)
    for block_number in range(N_FEAT):
        lower = block_number * block_width
        partial_value = jnp.dot(attended[:, lower:lower + block_width], out_weight[lower:lower + block_width, :], preferred_element_type=jnp.float32)
        partial_value = lax.optimization_barrier(partial_value.astype(jnp.bfloat16)).astype(jnp.float32)
        mixed_sum = mixed_sum + partial_value
    return mixed_sum.astype(jnp.bfloat16)
```

```python
import math
from functools import partial

import jax
import jax.numpy as jnp
from jax import lax
from jax.experimental import pallas as pl
from jax.experimental.pallas import tpu as pltpu
from jax.sharding import PartitionSpec as P

HD = 128
ROPE_BASE = 500000.0
NEG_FILL = -1e30
LONGEST = (5, 8)
FAR_BLOCKS = 7


def locate(token_index, doc_lengths):
    doc_ends = jnp.cumsum(doc_lengths)
    starts = doc_ends - doc_lengths
    doc_ids = jnp.sum((token_index[:, None] >= doc_ends[None, :]).astype(jnp.int32), axis=1)
    number = jnp.arange(doc_lengths.shape[0], dtype=jnp.int32)
    first_token = jnp.sum(
        jnp.where(doc_ids[:, None] == number[None, :], starts[None, :], 0), axis=1
    )
    return (doc_ids, token_index - first_token)


def tables(positions):
    half = HD // 2
    frequency = ROPE_BASE ** (-(jnp.arange(half, dtype=jnp.float32) * 2.0 / HD))
    angles = positions.astype(jnp.float32)[:, None] * frequency[None, :]
    cosine, sine = jnp.cos(angles), jnp.sin(angles)
    return (
        jnp.concatenate([cosine, cosine], axis=-1),
        jnp.concatenate([-sine, sine], axis=-1),
    )


def turn(block, cosine, sine):
    block = block.astype(jnp.float32)
    return (block * cosine + pltpu.roll(block, HD // 2, 1) * sine).astype(jnp.bfloat16)


def attention_kernel(first_ref, q_ref, k_ref, v_ref, *refs, reach, group):
    far = refs[:reach]
    cos_ref, sin_ref, start_ref, out_ref = refs[reach:]
    rows = q_ref.shape[0]
    kv_heads = k_ref.shape[1] // HD
    first = first_ref[0]
    scale = HD**-0.5 * math.log2(math.e)
    starts = start_ref[...]
    lane = lax.broadcasted_iota(jnp.int32, (rows, rows), 1)
    sub = lax.broadcasted_iota(jnp.int32, (rows, rows), 0)
    own_cos, own_sin = (r[reach * rows : (reach + 1) * rows, :] for r in (cos_ref, sin_ref))
    seen = []
    for d in range(reach, 0, -1):
        seen.append(first - d * rows + lane >= starts)
    seen.append((first + lane >= starts) & (lane <= sub))
    for g in range(kv_heads):
        at = slice(g * HD, (g + 1) * HD)
        keys, vals = [], []
        for d in range(reach, 0, -1):
            part = slice((reach - d) * rows, (reach - d + 1) * rows)
            keys.append(turn(far[d - 1][:, at], cos_ref[part, :], sin_ref[part, :]))
            vals.append(far[d - 1][:, kv_heads * HD + g * HD : kv_heads * HD + (g + 1) * HD])
        keys.append(turn(k_ref[:, at], own_cos, own_sin))
        vals.append(v_ref[:, at])
        keys = jnp.concatenate(keys, axis=0)
        vals = jnp.concatenate(vals, axis=0)
        for h in range(g * group, (g + 1) * group):
            query = turn(q_ref[:, h * HD : (h + 1) * HD], own_cos, own_sin)
            scores = lax.dot_general(
                query, keys, (((1,), (1,)), ((), ())), preferred_element_type=jnp.float32
            )
            masked = [
                jnp.where(seen[n], scores[:, n * rows : (n + 1) * rows] * scale, NEG_FILL)
                for n in range(reach + 1)
            ]
            top = masked[0]
            for m in masked[1:]:
                top = jnp.maximum(top, m)
            top = jnp.max(top, axis=1, keepdims=True)
            weights = [jnp.exp2(m - top) for m in masked]
            total = weights[0]
            for w in weights[1:]:
                total = total + w
            total = jnp.sum(total, axis=1, keepdims=True)
            rounded = jnp.concatenate([w.astype(jnp.bfloat16) for w in weights], axis=1)
            update = jnp.dot(rounded, vals, preferred_element_type=jnp.float32)
            out_ref[:, h * HD : (h + 1) * HD] = (update / total).astype(jnp.bfloat16)


def attend_near(queries, keys, values, doc_lengths, reach, n_tok):
    rows = queries.shape[0]
    me = lax.axis_index("tok")
    both = jnp.concatenate([keys, values], axis=1)
    far = []
    for d in range(1, reach + 1):
        far.append(lax.ppermute(both, "tok", [(i, i + d) for i in range(n_tok - d)]))
    first = me * rows
    window = first - reach * rows + jnp.arange((reach + 1) * rows, dtype=jnp.int32)
    _, positions = locate(window, doc_lengths)
    cosine, sine = tables(positions)
    starts = (window - positions)[reach * rows :].reshape(rows, 1)
    vmem = pl.BlockSpec(memory_space=pltpu.VMEM)
    attended = pl.pallas_call(
        partial(
            attention_kernel, reach=reach, group=queries.shape[1] // keys.shape[1]
        ),
        out_shape=jax.ShapeDtypeStruct(queries.shape, jnp.bfloat16),
        in_specs=[pl.BlockSpec(memory_space=pltpu.SMEM)] + [vmem] * (6 + reach),
        out_specs=vmem,
        name="attention",
    )(first.reshape(1), queries, keys, values, *far, cosine, sine, starts)
    return attended, far[-1]


def rotary(tensor, positions):
    half_size = tensor.shape[-1] // 2
    frequency = ROPE_BASE ** (-(jnp.arange(half_size, dtype=jnp.float32) * 2.0 / tensor.shape[-1]))
    angles = positions.astype(jnp.float32)[:, None] * frequency[None, :]
    cosine = jnp.cos(angles)[:, None, :]
    sine_part = jnp.sin(angles)[:, None, :]
    a = tensor[..., :half_size]
    b = tensor[..., half_size:]
    return jnp.concatenate([a * cosine - b * sine_part, b * cosine + a * sine_part], axis=-1)


def attend_far(queries, keys, values, doc_lengths):
    rows = queries.shape[0]
    heads, kv_heads = queries.shape[1] // HD, keys.shape[1] // HD
    own = lax.axis_index("tok") * rows + jnp.arange(rows, dtype=jnp.int32)
    docs, positions = locate(own, doc_lengths)
    rotated_q = rotary(queries.astype(jnp.float32).reshape(rows, heads, HD), positions)
    rotated_q = rotated_q.astype(jnp.bfloat16).reshape(rows, kv_heads, heads // kv_heads, HD)
    rotated_k = rotary(keys.astype(jnp.float32).reshape(rows, kv_heads, HD), positions)
    rotated_k = rotated_k.astype(jnp.bfloat16).reshape(rows, kv_heads * HD)
    all_k = lax.all_gather(rotated_k, "tok", axis=0, tiled=True)
    all_v = lax.all_gather(values, "tok", axis=0, tiled=True)
    step = 4 * rows

    def one_block(number, state):
        running, totals, weighted = state
        begin = number * step
        key = lax.dynamic_slice_in_dim(all_k, begin, step, 0).reshape(step, kv_heads, HD)
        value = lax.dynamic_slice_in_dim(all_v, begin, step, 0).reshape(step, kv_heads, HD)
        index = begin + jnp.arange(step, dtype=jnp.int32)
        key_docs, _ = locate(index, doc_lengths)
        scores = HD**-0.5 * jnp.einsum(
            "qgjd,kgd->gjqk", rotated_q, key, preferred_element_type=jnp.float32
        )
        visible = (docs[:, None] == key_docs[None, :]) & (index[None, :] <= own[:, None])
        scores = jnp.where(visible, scores, NEG_FILL)
        top = jnp.maximum(running, jnp.max(scores, axis=-1))
        factor = jnp.exp(running - top)
        weights = jnp.where(visible, jnp.exp(scores - top[..., None]), 0.0)
        totals = totals * factor + jnp.sum(weights, axis=-1)
        update = jnp.einsum(
            "gjqk,kgd->gjqd",
            weights.astype(jnp.bfloat16),
            value,
            preferred_element_type=jnp.float32,
        )
        return (top, totals, weighted * factor[..., None] + update)

    shape = (kv_heads, heads // kv_heads, rows)
    state = (
        jnp.full(shape, NEG_FILL, jnp.float32),
        jnp.zeros(shape, jnp.float32),
        jnp.zeros(shape + (HD,), jnp.float32),
    )
    _, totals, weighted = lax.fori_loop(0, all_k.shape[0] // step, one_block, state)
    output = (weighted / totals[..., None]).transpose(2, 0, 1, 3)
    return output.reshape(rows, heads * HD).astype(jnp.bfloat16), all_v[:rows]


def project_kernel(place_ref, *refs, count, sides):
    blocks, weights, (keep_ref, send_ref) = refs[:count], refs[count:-2], refs[-2:]
    width = weights[0].shape[1]
    for r in range(count):
        pieces = [
            jnp.dot(blocks[r][...], w[...], preferred_element_type=jnp.float32).astype(jnp.bfloat16)
            for w in weights
        ]
        slot = r ^ place_ref[1]
        turn_now = slot & 1
        for n, piece in enumerate(pieces):
            begin = pl.multiple_of((place_ref[0] ^ n) * width if sides > 1 else 0, HD)

            @pl.when(slot < count // 2)
            def _():
                keep_ref[turn_now, :, pl.ds(begin, width)] = piece

            @pl.when(slot >= count // 2)
            def _():
                send_ref[turn_now, :, pl.ds(begin, width)] = piece


def solution(mesh):
    n_tok, n_feat = mesh.shape["tok"], mesh.shape["feat"]
    inner = n_tok // n_feat

    def everyone(move):
        pairs = []
        for z in range(n_feat):
            for x in range(inner):
                for j in range(n_feat):
                    to_z, to_x, to_j = move(z, x, j)
                    pairs.append(
                        (
                            (z * inner + x) * n_feat + j,
                            (to_z * inner + to_x) * n_feat + to_j,
                        )
                    )
        return pairs

    def permute(array, move):
        return lax.ppermute(array, ("tok", "feat"), everyone(move))

    def shards(queries, keys, values, out_weight, doc_lengths):
        rows = queries.shape[0]
        me, feat = lax.axis_index("tok"), lax.axis_index("feat")
        z, x = me // inner, me % inner
        longest = n_tok * rows * LONGEST[0] // LONGEST[1]
        reach = min(n_tok - 1, -(-(longest - 1) // rows))
        if reach <= FAR_BLOCKS:
            attended, seen = attend_near(queries, keys, values, doc_lengths, reach, n_tok)
        else:
            attended, seen = attend_far(queries, keys, values, doc_lengths)
        out_weight, _ = lax.optimization_barrier((out_weight, seen))
        if inner == 2:
            weights = [out_weight, permute(out_weight, lambda z, x, j: (z, 1 - x, j))]
        else:
            groups = [[z * inner + x for x in range(inner)] for z in range(n_feat)]
            weights = [
                lax.all_gather(
                    out_weight, "tok", axis=1, tiled=True, axis_index_groups=groups
                )
            ]
        blocks = [attended] + [
            permute(attended, lambda z, x, j, r=r: (z ^ r, x, j)) for r in range(1, n_feat)
        ]
        low, high = feat & 1, feat >> 1
        mask = low * 2 + high
        place = jnp.stack([x, mask]).astype(jnp.int32)
        vmem = pl.BlockSpec(memory_space=pltpu.VMEM)
        half = jax.ShapeDtypeStruct(
            (n_feat // 2, rows, sum(w.shape[1] for w in weights)), jnp.bfloat16
        )
        keep, send = pl.pallas_call(
            partial(project_kernel, count=n_feat, sides=len(weights)),
            out_shape=(half, half),
            in_specs=[pl.BlockSpec(memory_space=pltpu.SMEM)] + [vmem] * (n_feat + len(weights)),
            out_specs=(vmem, vmem),
            name="project",
        )(place, *blocks, *weights)
        other = permute(send, lambda z, x, j: (z, x, j ^ 1))
        both = keep.astype(jnp.float32) + other.astype(jnp.float32)
        both = both.astype(jnp.bfloat16)
        home = [
            permute(
                both[k],
                lambda z, x, j, k=k: (z ^ ((j & 1) * 2 + ((j >> 1) ^ k)), x, z),
            )
            for k in range(2)
        ]
        return (home[0].astype(jnp.float32) + home[1].astype(jnp.float32)).astype(jnp.bfloat16)

    in_specs = (P("tok", "feat"), P("tok", "feat"), P("tok", "feat"), P("feat", "tok"), P())
    return jax.shard_map(
        shards, mesh=mesh, in_specs=in_specs, out_specs=P("tok", "feat"), check_vma=False
    )
```

```python
import math
from functools import partial

import jax
import jax.numpy as jnp
from jax import lax
from jax.experimental import pallas as pl
from jax.experimental.pallas import tpu as pltpu
from jax.sharding import PartitionSpec as P


HD = 128
ROPE_BASE = 500000.0
NEG_FILL = -1e30
LONGEST = (5, 8)
KERNEL_BYTES = 16 << 20
FAR_BLOCKS = 7


def locate(token_index, doc_lengths):
    doc_ends = jnp.cumsum(doc_lengths)
    starts = doc_ends - doc_lengths
    doc_ids = jnp.sum((token_index[:, None] >= doc_ends[None, :]).astype(jnp.int32), axis=1)
    number = jnp.arange(doc_lengths.shape[0], dtype=jnp.int32)
    first_token = jnp.sum(
        jnp.where(doc_ids[:, None] == number[None, :], starts[None, :], 0), axis=1
    )
    return (doc_ids, token_index - first_token)


def on_chip(*arrays):
    return [pltpu.with_memory_space_constraint(a, pltpu.VMEM) for a in arrays]


def sine_cosine(angle):
    turns = jnp.round(angle * (2.0 / math.pi))
    rest = ((angle - turns * 1.5703125) - turns * 4.837512969970703125e-4) - turns * 7.54978995489188216e-8
    square = rest * rest
    sine = (-1.9515295891e-4 * square + 8.3321608736e-3) * square - 1.6666654611e-1
    sine = sine * square * rest + rest
    cosine = (2.443315711809948e-5 * square - 1.388731625493765e-3) * square
    cosine = (cosine + 4.166664568298827e-2) * square * square - 0.5 * square + 1.0
    quarter = turns.astype(jnp.int32)
    swapped = (quarter & 1) == 1
    flip_sine = (quarter & 2) == 2
    flip_cosine = ((quarter + 1) & 2) == 2
    out_sine = jnp.where(swapped, cosine, sine)
    out_cosine = jnp.where(swapped, sine, cosine)
    return (
        jnp.where(flip_sine, -out_sine, out_sine),
        jnp.where(flip_cosine, -out_cosine, out_cosine),
    )


def doc_start(index, lengths_ref):
    start, end = jnp.zeros_like(index), jnp.int32(0)
    for n in range(lengths_ref.shape[0]):
        start = jnp.where(index >= end, end, start)
        end = end + lengths_ref[n]
    return start


def turn(block, cosine, sine):
    block = block.astype(jnp.float32)
    return (block * cosine + pltpu.roll(block, HD // 2, 1) * sine).astype(jnp.bfloat16)


def attention_kernel(first_ref, lengths_ref, freq_ref, q_ref, k_ref, v_ref, *refs, reach, group):
    far, (out_ref, copy_ref, score_ref, weight_ref) = refs[:reach], refs[reach:]
    rows = q_ref.shape[0]
    kv_heads = k_ref.shape[1] // HD
    count = reach + 1
    first = first_ref[0]
    scale = HD**-0.5 * math.log2(math.e)
    lane = lax.broadcasted_iota(jnp.int32, (rows, HD), 1)
    sub = lax.broadcasted_iota(jnp.int32, (rows, HD), 0)
    freq = freq_ref[...]
    cosines, sines = [], []
    for n in range(count):
        index = first - (reach - n) * rows + sub
        start = doc_start(index, lengths_ref)
        sine, cosine = sine_cosine((index - start).astype(jnp.float32) * freq)
        cosines.append(cosine)
        sines.append(jnp.where(lane < HD // 2, -sine, sine))
    key_lane = lax.broadcasted_iota(jnp.int32, (rows, rows), 1)
    key_sub = lax.broadcasted_iota(jnp.int32, (rows, rows), 0)
    starts = doc_start(first + key_sub, lengths_ref)
    seen = [first - (reach - n) * rows + key_lane >= starts for n in range(count)]
    seen[reach] = seen[reach] & (key_lane <= key_sub)
    for g in range(kv_heads):
        at = slice(g * HD, (g + 1) * HD)
        at_v = slice((kv_heads + g) * HD, (kv_heads + g + 1) * HD)
        keys = [turn(far[reach - n - 1][:, at], cosines[n], sines[n]) for n in range(reach)]
        keys = jnp.concatenate(keys + [turn(k_ref[:, at], cosines[reach], sines[reach])], axis=0)
        vals = jnp.concatenate(
            [far[reach - n - 1][:, at_v] for n in range(reach)] + [v_ref[:, at]], axis=0
        )
        query = jnp.concatenate(
            [
                turn(q_ref[:, h * HD : (h + 1) * HD], cosines[reach], sines[reach])
                for h in range(g * group, (g + 1) * group)
            ],
            axis=0,
        )
        score_ref[...] = lax.dot_general(
            query, keys, (((1,), (1,)), ((), ())), preferred_element_type=jnp.float32
        )
        totals = []
        for h in range(group):
            band = slice(h * rows, (h + 1) * rows)
            masked = [
                jnp.where(seen[n], score_ref[band, n * rows : (n + 1) * rows] * scale, NEG_FILL)
                for n in range(count)
            ]
            top = masked[0]
            for m in masked[1:]:
                top = jnp.maximum(top, m)
            top = jnp.max(top, axis=1, keepdims=True)
            total = None
            for n in range(count):
                w = jnp.exp2(masked[n] - top)
                total = w if total is None else total + w
                weight_ref[band, n * rows : (n + 1) * rows] = w.astype(jnp.bfloat16)
            totals.append(jnp.sum(total, axis=1, keepdims=True))
        update = jnp.dot(weight_ref[...], vals, preferred_element_type=jnp.float32)
        for h in range(group):
            piece = update[h * rows : (h + 1) * rows, :] / totals[h]
            head = g * group + h
            out_ref[:, head * HD : (head + 1) * HD] = piece.astype(jnp.bfloat16)
            copy_ref[:, head * HD : (head + 1) * HD] = piece.astype(jnp.bfloat16)


def attend_near(queries, keys, values, doc_lengths, reach, n_tok):
    rows = queries.shape[0]
    group = queries.shape[1] // keys.shape[1]
    both = jnp.concatenate([keys, values], axis=1)
    far = []
    for d in range(1, reach + 1):
        far.append(lax.ppermute(both, "tok", [(i, i + d) for i in range(n_tok - d)]))
    first = (lax.axis_index("tok") * rows).astype(jnp.int32).reshape(1)
    half = jnp.arange(HD, dtype=jnp.float32) % (HD // 2)
    freq = (ROPE_BASE ** (-(half * 2.0 / HD))).reshape(1, HD)
    vmem = pl.BlockSpec(memory_space=pltpu.VMEM)
    smem = pl.BlockSpec(memory_space=pltpu.SMEM)
    span = (reach + 1) * rows
    attended = pl.pallas_call(
        partial(attention_kernel, reach=reach, group=group),
        out_shape=(pltpu.VMEM(queries.shape, jnp.bfloat16),) * 2,
        in_specs=[smem, smem] + [vmem] * (4 + reach),
        out_specs=(vmem, vmem),
        scratch_shapes=[
            pltpu.VMEM((group * rows, span), jnp.float32),
            pltpu.VMEM((group * rows, span), jnp.bfloat16),
        ],
        compiler_params=pltpu.CompilerParams(vmem_limit_bytes=KERNEL_BYTES),
        name="attention",
    )(first, doc_lengths, freq, *on_chip(queries, keys, values, *far))
    return *attended, far


def rotary(tensor, positions):
    half_size = tensor.shape[-1] // 2
    frequency = ROPE_BASE ** (-(jnp.arange(half_size, dtype=jnp.float32) * 2.0 / tensor.shape[-1]))
    angles = positions.astype(jnp.float32)[:, None] * frequency[None, :]
    cosine = jnp.cos(angles)[:, None, :]
    sine_part = jnp.sin(angles)[:, None, :]
    a = tensor[..., :half_size]
    b = tensor[..., half_size:]
    return jnp.concatenate([a * cosine - b * sine_part, b * cosine + a * sine_part], axis=-1)


def attend_far(queries, keys, values, doc_lengths):
    rows = queries.shape[0]
    heads, kv_heads = queries.shape[1] // HD, keys.shape[1] // HD
    own = lax.axis_index("tok") * rows + jnp.arange(rows, dtype=jnp.int32)
    docs, positions = locate(own, doc_lengths)
    rotated_q = rotary(queries.astype(jnp.float32).reshape(rows, heads, HD), positions)
    rotated_q = rotated_q.astype(jnp.bfloat16).reshape(rows, kv_heads, heads // kv_heads, HD)
    rotated_k = rotary(keys.astype(jnp.float32).reshape(rows, kv_heads, HD), positions)
    rotated_k = rotated_k.astype(jnp.bfloat16).reshape(rows, kv_heads * HD)
    all_k = lax.all_gather(rotated_k, "tok", axis=0, tiled=True)
    all_v = lax.all_gather(values, "tok", axis=0, tiled=True)
    step = 4 * rows

    def one_block(number, state):
        running, totals, weighted = state
        begin = number * step
        key = lax.dynamic_slice_in_dim(all_k, begin, step, 0).reshape(step, kv_heads, HD)
        value = lax.dynamic_slice_in_dim(all_v, begin, step, 0).reshape(step, kv_heads, HD)
        index = begin + jnp.arange(step, dtype=jnp.int32)
        key_docs, _ = locate(index, doc_lengths)
        scores = HD**-0.5 * jnp.einsum(
            "qgjd,kgd->gjqk", rotated_q, key, preferred_element_type=jnp.float32
        )
        visible = (docs[:, None] == key_docs[None, :]) & (index[None, :] <= own[:, None])
        scores = jnp.where(visible, scores, NEG_FILL)
        top = jnp.maximum(running, jnp.max(scores, axis=-1))
        factor = jnp.exp(running - top)
        weights = jnp.where(visible, jnp.exp(scores - top[..., None]), 0.0)
        totals = totals * factor + jnp.sum(weights, axis=-1)
        update = jnp.einsum(
            "gjqk,kgd->gjqd",
            weights.astype(jnp.bfloat16),
            value,
            preferred_element_type=jnp.float32,
        )
        return (top, totals, weighted * factor[..., None] + update)

    shape = (kv_heads, heads // kv_heads, rows)
    state = (
        jnp.full(shape, NEG_FILL, jnp.float32),
        jnp.zeros(shape, jnp.float32),
        jnp.zeros(shape + (HD,), jnp.float32),
    )
    _, totals, weighted = lax.fori_loop(0, all_k.shape[0] // step, one_block, state)
    output = (weighted / totals[..., None]).transpose(2, 0, 1, 3)
    output = output.reshape(rows, heads * HD).astype(jnp.bfloat16)
    return output, output, all_v[0]


def columns(left, weights, flip):
    pieces = []
    for w in weights:
        piece = jnp.dot(left, w[...], preferred_element_type=jnp.float32)
        pieces.append(piece.astype(jnp.bfloat16))
    if len(pieces) == 1:
        return pieces[0]
    straight = jnp.concatenate(pieces, axis=1)
    return jnp.where(flip == 0, straight, jnp.concatenate(pieces[::-1], axis=1))


def near_kernel(place_ref, own_ref, mate_ref, *refs, sides):
    weights, (first_ref, second_ref) = refs[:sides], refs[sides : sides + 2]
    rows = own_ref.shape[0]
    left = jnp.concatenate([own_ref[...], mate_ref[...]], axis=0)
    result = columns(left, weights, place_ref[0])
    own, mate = result[:rows], result[rows:]
    first_ref[...] = jnp.where(place_ref[1] == 0, own, mate)
    second_ref[...] = jnp.where(place_ref[1] == 0, mate, own)


def away_kernel(place_ref, near_ref, far_ref, *refs, sides):
    weights, (keep_ref, send_ref) = refs[:sides], refs[sides : sides + 2]
    result = columns(far_ref[...], weights, place_ref[0])
    keep_ref[...] = jnp.where(place_ref[2] == 0, near_ref[...], result)
    send_ref[...] = jnp.where(place_ref[2] == 0, result, near_ref[...])


def project(kernel, place, left, weights):
    rows, width = left[0].shape[0], sum(w.shape[1] for w in weights)
    vmem = pl.BlockSpec(memory_space=pltpu.VMEM)
    outs = [pltpu.VMEM((rows, width), jnp.bfloat16)] * 2
    outs += [pltpu.VMEM(w.shape, w.dtype) for w in weights]
    begin = 1 + len(left)
    first, second, *weights = pl.pallas_call(
        partial(kernel, sides=len(weights)),
        out_shape=tuple(outs),
        in_specs=[pl.BlockSpec(memory_space=pltpu.SMEM)] + [vmem] * (len(left) + len(weights)),
        out_specs=(vmem,) * len(outs),
        input_output_aliases={begin + n: 2 + n for n in range(len(weights))},
        compiler_params=pltpu.CompilerParams(vmem_limit_bytes=KERNEL_BYTES),
    )(place, *on_chip(*left, *weights))
    return first, second, weights


def solution(mesh):
    n_tok, n_feat = mesh.shape["tok"], mesh.shape["feat"]
    inner = n_tok // n_feat

    def everyone(move):
        pairs = []
        for z in range(n_feat):
            for x in range(inner):
                for j in range(n_feat):
                    to_z, to_x, to_j = move(z, x, j)
                    pairs.append(
                        (
                            (z * inner + x) * n_feat + j,
                            (to_z * inner + to_x) * n_feat + to_j,
                        )
                    )
        return pairs

    def permute(array, move):
        return lax.ppermute(array, ("tok", "feat"), everyone(move))

    def shards(queries, keys, values, out_weight, doc_lengths):
        rows = queries.shape[0]
        me, feat = lax.axis_index("tok"), lax.axis_index("feat")
        x = me % inner
        longest = n_tok * rows * LONGEST[0] // LONGEST[1]
        reach = min(n_tok - 1, -(-(longest - 1) // rows))
        if reach <= FAR_BLOCKS:
            attended, own, seen = attend_near(queries, keys, values, doc_lengths, reach, n_tok)
        else:
            attended, own, seen = attend_far(queries, keys, values, doc_lengths)
        out_weight, _ = lax.optimization_barrier((out_weight, seen))
        if inner == 2:
            weights = [out_weight, permute(out_weight, lambda z, x, j: (z, 1 - x, j))]
        else:
            groups = [[z * inner + x for x in range(inner)] for z in range(n_feat)]
            weights = [
                lax.all_gather(
                    out_weight, "tok", axis=1, tiled=True, axis_index_groups=groups
                )
            ]
        mate = permute(attended, lambda z, x, j: (z ^ 1, x, j))
        away = []
        for k in range(2):
            away.append(
                permute(attended, lambda z, x, j: (z ^ (2 | ((j >> 1) ^ k)), x, j))
            )
        place = jnp.stack([x, feat >> 1, feat & 1]).astype(jnp.int32)
        *near, weights = project(near_kernel, place, [own, mate], weights)
        home = []
        for k in range(2):
            keep, send, weights = project(away_kernel, place, [near[k], away[k]], weights)
            other = permute(send, lambda z, x, j: (z, x, j ^ 1))
            both = (keep.astype(jnp.float32) + other.astype(jnp.float32)).astype(jnp.bfloat16)
            home.append(permute(both, lambda z, x, j: (z ^ ((j & 1) * 2 + ((j >> 1) ^ k)), x, z)))
        return (home[0].astype(jnp.float32) + home[1].astype(jnp.float32)).astype(jnp.bfloat16)

    in_specs = (P("tok", "feat"), P("tok", "feat"), P("tok", "feat"), P("feat", "tok"), P())
    return jax.shard_map(
        shards, mesh=mesh, in_specs=in_specs, out_specs=P("tok", "feat"), check_vma=False
    )
```

```python
import math
from functools import partial

import jax
import jax.numpy as jnp
import numpy as np
from jax import lax
from jax.experimental import pallas as pl
from jax.experimental.pallas import tpu as pltpu
from jax.sharding import PartitionSpec as P


HD = 128
ROPE_BASE = 500000.0
NEG_FILL = -1e30
LONGEST = (5, 8)
KERNEL_BYTES = 16 << 20
FAR_BLOCKS = 7


def locate(token_index, doc_lengths):
    doc_ends = jnp.cumsum(doc_lengths)
    starts = doc_ends - doc_lengths
    doc_ids = jnp.sum((token_index[:, None] >= doc_ends[None, :]).astype(jnp.int32), axis=1)
    number = jnp.arange(doc_lengths.shape[0], dtype=jnp.int32)
    first_token = jnp.sum(
        jnp.where(doc_ids[:, None] == number[None, :], starts[None, :], 0), axis=1
    )
    return (doc_ids, token_index - first_token)


def on_chip(*arrays):
    return [pltpu.with_memory_space_constraint(a, pltpu.VMEM) for a in arrays]


def sine_cosine(angle):
    turns = jnp.round(angle * (2.0 / math.pi))
    rest = ((angle - turns * 1.5703125) - turns * 4.837512969970703125e-4) - turns * 7.54978995489188216e-8
    square = rest * rest
    sine = (-1.9515295891e-4 * square + 8.3321608736e-3) * square - 1.6666654611e-1
    sine = sine * square * rest + rest
    cosine = (2.443315711809948e-5 * square - 1.388731625493765e-3) * square
    cosine = (cosine + 4.166664568298827e-2) * square * square - 0.5 * square + 1.0
    quarter = turns.astype(jnp.int32)
    swapped = (quarter & 1) == 1
    flip_sine = (quarter & 2) == 2
    flip_cosine = ((quarter + 1) & 2) == 2
    out_sine = jnp.where(swapped, cosine, sine)
    out_cosine = jnp.where(swapped, sine, cosine)
    return (
        jnp.where(flip_sine, -out_sine, out_sine),
        jnp.where(flip_cosine, -out_cosine, out_cosine),
    )


def doc_start(index, lengths_ref):
    start, end = jnp.zeros_like(index), jnp.int32(0)
    for n in range(lengths_ref.shape[0]):
        start = jnp.where(index >= end, end, start)
        end = end + lengths_ref[n]
    return start


def turn(block, cosine, sine):
    block = block.astype(jnp.float32)
    return (block * cosine + pltpu.roll(block, HD // 2, 1) * sine).astype(jnp.bfloat16)


def prepare_kernel(lengths_ref, freq_ref, q_ref, k_ref, *refs, reach):
    cos_ref, sin_ref, query_ref, key_ref = refs
    rows = k_ref.shape[0]
    first = lax.axis_index("tok") * rows
    lane = lax.broadcasted_iota(jnp.int32, (rows, HD), 1)
    sub = lax.broadcasted_iota(jnp.int32, (rows, HD), 0)
    freq = freq_ref[...]
    for n in range(reach + 1):
        index = first - (reach - n) * rows + sub
        start = doc_start(index, lengths_ref)
        sine, cosine = sine_cosine((index - start).astype(jnp.float32) * freq)
        sine = jnp.where(lane < HD // 2, -sine, sine)
        if n < reach:
            cos_ref[n * rows : (n + 1) * rows, :] = cosine
            sin_ref[n * rows : (n + 1) * rows, :] = sine
    for source, target in ((q_ref, query_ref), (k_ref, key_ref)):
        for h in range(source.shape[1] // HD):
            at = slice(h * HD, (h + 1) * HD)
            target[:, at] = turn(source[:, at], cosine, sine)


def attention_kernel(lengths_ref, cos_ref, sin_ref, q_ref, k_ref, v_ref, *refs, reach):
    far, (out_ref, score_ref, weight_ref) = refs[:reach], refs[reach:]
    rows = k_ref.shape[0]
    kv_heads = k_ref.shape[1] // HD
    group = q_ref.shape[1] // k_ref.shape[1]
    count = reach + 1
    first = lax.axis_index("tok") * rows
    scale = HD**-0.5 * math.log2(math.e)
    key_lane = lax.broadcasted_iota(jnp.int32, (rows, rows), 1)
    key_sub = lax.broadcasted_iota(jnp.int32, (rows, rows), 0)
    starts = doc_start(first + key_sub, lengths_ref)
    seen = [first - (reach - n) * rows + key_lane >= starts for n in range(count)]
    seen[reach] = seen[reach] & (key_lane <= key_sub)
    for g in range(kv_heads):
        at = slice(g * HD, (g + 1) * HD)
        at_v = slice((kv_heads + g) * HD, (kv_heads + g + 1) * HD)
        keys = []
        for n in range(reach):
            part = slice(n * rows, (n + 1) * rows)
            keys.append(turn(far[reach - n - 1][:, at], cos_ref[part, :], sin_ref[part, :]))
        keys = jnp.concatenate(keys + [k_ref[:, at]], axis=0)
        vals = jnp.concatenate(
            [far[reach - n - 1][:, at_v] for n in range(reach)] + [v_ref[:, at]], axis=0
        )
        query = jnp.concatenate(
            [q_ref[:, h * HD : (h + 1) * HD] for h in range(g * group, (g + 1) * group)], axis=0
        )
        score_ref[g] = lax.dot_general(
            query, keys, (((1,), (1,)), ((), ())), preferred_element_type=jnp.float32
        )
        totals = []
        for h in range(group):
            band = slice(h * rows, (h + 1) * rows)
            masked = [
                jnp.where(seen[n], score_ref[g, band, n * rows : (n + 1) * rows] * scale, NEG_FILL)
                for n in range(count)
            ]
            top = masked[0]
            for m in masked[1:]:
                top = jnp.maximum(top, m)
            top = jnp.max(top, axis=1, keepdims=True)
            total = None
            for n in range(count):
                w = jnp.exp2(masked[n] - top)
                total = w if total is None else total + w
                weight_ref[g, band, n * rows : (n + 1) * rows] = w.astype(jnp.bfloat16)
            totals.append(jnp.sum(total, axis=1, keepdims=True))
        update = jnp.dot(weight_ref[g], vals, preferred_element_type=jnp.float32)
        for h in range(group):
            piece = update[h * rows : (h + 1) * rows, :] / totals[h]
            head = g * group + h
            out_ref[:, head * HD : (head + 1) * HD] = piece.astype(jnp.bfloat16)


def attend_near(queries, keys, values, doc_lengths, reach, n_tok):
    rows = queries.shape[0]
    kv_heads = keys.shape[1] // HD
    group = queries.shape[1] // keys.shape[1]
    both = jnp.concatenate([keys, values], axis=1)
    far = []
    for d in range(1, reach + 1):
        far.append(lax.ppermute(both, "tok", [(i, i + d) for i in range(n_tok - d)]))
    half = np.arange(HD, dtype=np.float32) % (HD // 2)
    freq = jnp.asarray((ROPE_BASE ** (-(half * 2.0 / HD))).astype(np.float32).reshape(1, HD))
    vmem = pl.BlockSpec(memory_space=pltpu.VMEM)
    smem = pl.BlockSpec(memory_space=pltpu.SMEM)
    span = (reach + 1) * rows
    whole = pltpu.VMEM(queries.shape, jnp.bfloat16)
    settings = pltpu.CompilerParams(vmem_limit_bytes=KERNEL_BYTES)
    cosine, sine, query, key = pl.pallas_call(
        partial(prepare_kernel, reach=reach),
        out_shape=(
            pltpu.VMEM((reach * rows, HD), jnp.float32),
            pltpu.VMEM((reach * rows, HD), jnp.float32),
            whole,
            pltpu.VMEM(keys.shape, jnp.bfloat16),
        ),
        in_specs=[smem] + [vmem] * 3,
        out_specs=(vmem,) * 4,
        compiler_params=settings,
        name="prepare",
    )(doc_lengths, freq, *on_chip(queries, keys))
    return pl.pallas_call(
        partial(attention_kernel, reach=reach),
        out_shape=whole,
        in_specs=[smem] + [vmem] * (5 + reach),
        out_specs=vmem,
        scratch_shapes=[
            pltpu.VMEM((kv_heads, group * rows, span), jnp.float32),
            pltpu.VMEM((kv_heads, group * rows, span), jnp.bfloat16),
        ],
        compiler_params=settings,
        name="attention",
    )(doc_lengths, *on_chip(cosine, sine, query, key, values, *far))


def rotary(tensor, positions):
    half_size = tensor.shape[-1] // 2
    frequency = ROPE_BASE ** (-(jnp.arange(half_size, dtype=jnp.float32) * 2.0 / tensor.shape[-1]))
    angles = positions.astype(jnp.float32)[:, None] * frequency[None, :]
    cosine = jnp.cos(angles)[:, None, :]
    sine_part = jnp.sin(angles)[:, None, :]
    a = tensor[..., :half_size]
    b = tensor[..., half_size:]
    return jnp.concatenate([a * cosine - b * sine_part, b * cosine + a * sine_part], axis=-1)


def attend_far(queries, keys, values, doc_lengths):
    rows = queries.shape[0]
    heads, kv_heads = queries.shape[1] // HD, keys.shape[1] // HD
    own = lax.axis_index("tok") * rows + jnp.arange(rows, dtype=jnp.int32)
    docs, positions = locate(own, doc_lengths)
    rotated_q = rotary(queries.astype(jnp.float32).reshape(rows, heads, HD), positions)
    rotated_q = rotated_q.astype(jnp.bfloat16).reshape(rows, kv_heads, heads // kv_heads, HD)
    rotated_k = rotary(keys.astype(jnp.float32).reshape(rows, kv_heads, HD), positions)
    rotated_k = rotated_k.astype(jnp.bfloat16).reshape(rows, kv_heads * HD)
    all_k = lax.all_gather(rotated_k, "tok", axis=0, tiled=True)
    all_v = lax.all_gather(values, "tok", axis=0, tiled=True)
    step = 4 * rows

    def one_block(number, state):
        running, totals, weighted = state
        begin = number * step
        key = lax.dynamic_slice_in_dim(all_k, begin, step, 0).reshape(step, kv_heads, HD)
        value = lax.dynamic_slice_in_dim(all_v, begin, step, 0).reshape(step, kv_heads, HD)
        index = begin + jnp.arange(step, dtype=jnp.int32)
        key_docs, _ = locate(index, doc_lengths)
        scores = HD**-0.5 * jnp.einsum(
            "qgjd,kgd->gjqk", rotated_q, key, preferred_element_type=jnp.float32
        )
        visible = (docs[:, None] == key_docs[None, :]) & (index[None, :] <= own[:, None])
        scores = jnp.where(visible, scores, NEG_FILL)
        top = jnp.maximum(running, jnp.max(scores, axis=-1))
        factor = jnp.exp(running - top)
        weights = jnp.where(visible, jnp.exp(scores - top[..., None]), 0.0)
        totals = totals * factor + jnp.sum(weights, axis=-1)
        update = jnp.einsum(
            "gjqk,kgd->gjqd",
            weights.astype(jnp.bfloat16),
            value,
            preferred_element_type=jnp.float32,
        )
        return (top, totals, weighted * factor[..., None] + update)

    shape = (kv_heads, heads // kv_heads, rows)
    state = (
        jnp.full(shape, NEG_FILL, jnp.float32),
        jnp.zeros(shape, jnp.float32),
        jnp.zeros(shape + (HD,), jnp.float32),
    )
    _, totals, weighted = lax.fori_loop(0, all_k.shape[0] // step, one_block, state)
    output = (weighted / totals[..., None]).transpose(2, 0, 1, 3)
    return output.reshape(rows, heads * HD).astype(jnp.bfloat16)


def project_kernel(own_ref, mate_ref, *refs, inner):
    half = (len(refs) - 1) // 2
    out_ref = refs[-1]
    pieces = []
    for own_w, mate_w in zip(refs[:half], refs[half:-1]):
        own = jnp.dot(own_ref[...], own_w[...], preferred_element_type=jnp.float32)
        mate = jnp.dot(mate_ref[...], mate_w[...], preferred_element_type=jnp.float32)
        own, mate = (p.astype(jnp.bfloat16).astype(jnp.float32) for p in (own, mate))
        pieces.append((own + mate).astype(jnp.bfloat16))
    straight = jnp.concatenate(pieces, axis=1)
    if half > 1:
        flip = lax.rem(lax.axis_index("tok"), inner)
        straight = jnp.where(flip == 0, straight, jnp.concatenate(pieces[::-1], axis=1))
    out_ref[...] = straight


def project(inner, own, mate, own_weights, mate_weights):
    vmem = pl.BlockSpec(memory_space=pltpu.VMEM)
    operands = on_chip(own, mate, *own_weights, *mate_weights)
    return pl.pallas_call(
        partial(project_kernel, inner=inner),
        out_shape=pltpu.VMEM((own.shape[0], sum(w.shape[1] for w in own_weights)), jnp.bfloat16),
        in_specs=[vmem] * len(operands),
        out_specs=vmem,
        compiler_params=pltpu.CompilerParams(vmem_limit_bytes=KERNEL_BYTES),
    )(*operands)


def solution(mesh):
    n_tok, n_feat = mesh.shape["tok"], mesh.shape["feat"]
    inner = n_tok // n_feat

    def everyone(move):
        pairs = []
        for z in range(n_feat):
            for x in range(inner):
                for j in range(n_feat):
                    to_z, to_x, to_j = move(z, x, j)
                    pairs.append(
                        (
                            (z * inner + x) * n_feat + j,
                            (to_z * inner + to_x) * n_feat + to_j,
                        )
                    )
        return pairs

    def permute(array, move):
        return lax.ppermute(array, ("tok", "feat"), everyone(move))

    def shards(queries, keys, values, out_weight, doc_lengths):
        rows = queries.shape[0]
        longest = n_tok * rows * LONGEST[0] // LONGEST[1]
        reach = min(n_tok - 1, -(-(longest - 1) // rows))
        if reach <= FAR_BLOCKS:
            attended = attend_near(queries, keys, values, doc_lengths, reach, n_tok)
        else:
            attended = attend_far(queries, keys, values, doc_lengths)
        if inner == 2:
            weights = [out_weight, permute(out_weight, lambda z, x, j: (z, 1 - x, j))]
        else:
            groups = [[z * inner + x for x in range(inner)] for z in range(n_feat)]
            weights = [
                lax.all_gather(
                    out_weight, "tok", axis=1, tiled=True, axis_index_groups=groups
                )
            ]
        mate_weights = []
        for w in weights:
            mate_weights.append(permute(w, lambda z, x, j: (z, x, j ^ 1)))

        def deliver(k, cross):
            def move(z, x, j):
                core = (j & 1) ^ cross
                return (z ^ (core * 2 | ((j >> 1) ^ k)), x, (j & 2) | core)

            return permute(attended, move)

        home = []
        for k in range(2):
            own, mate = deliver(k, 0), deliver(k, 1)
            mixed = project(inner, own, mate, weights, mate_weights)
            home.append(permute(mixed, lambda z, x, j: (z ^ ((j & 1) * 2 + ((j >> 1) ^ k)), x, z)))
        return (home[0].astype(jnp.float32) + home[1].astype(jnp.float32)).astype(jnp.bfloat16)

    in_specs = (P("tok", "feat"), P("tok", "feat"), P("tok", "feat"), P("feat", "tok"), P())
    return jax.shard_map(
        shards, mesh=mesh, in_specs=in_specs, out_specs=P("tok", "feat"), check_vma=False
    )
```

```python
import math
from functools import partial

import jax
import jax.numpy as jnp
import numpy as np
from jax import lax
from jax.experimental import pallas as pl
from jax.experimental.pallas import tpu as pltpu
from jax.sharding import PartitionSpec as P


HD = 128
ROPE_BASE = 500000.0
NEG_FILL = -1e30
LONGEST = (5, 8)
KERNEL_BYTES = 16 << 20
FAR_BLOCKS = 7


def locate(token_index, doc_lengths):
    doc_ends = jnp.cumsum(doc_lengths)
    starts = doc_ends - doc_lengths
    doc_ids = jnp.sum((token_index[:, None] >= doc_ends[None, :]).astype(jnp.int32), axis=1)
    number = jnp.arange(doc_lengths.shape[0], dtype=jnp.int32)
    first_token = jnp.sum(
        jnp.where(doc_ids[:, None] == number[None, :], starts[None, :], 0), axis=1
    )
    return (doc_ids, token_index - first_token)


def on_chip(*arrays):
    return [pltpu.with_memory_space_constraint(a, pltpu.VMEM) for a in arrays]


def sine_cosine(angle):
    turns = jnp.round(angle * (2.0 / math.pi))
    rest = ((angle - turns * 1.5703125) - turns * 4.837512969970703125e-4) - turns * 7.54978995489188216e-8
    square = rest * rest
    sine = (-1.9515295891e-4 * square + 8.3321608736e-3) * square - 1.6666654611e-1
    sine = sine * square * rest + rest
    cosine = (2.443315711809948e-5 * square - 1.388731625493765e-3) * square
    cosine = (cosine + 4.166664568298827e-2) * square * square - 0.5 * square + 1.0
    quarter = turns.astype(jnp.int32)
    swapped = (quarter & 1) == 1
    flip_sine = (quarter & 2) == 2
    flip_cosine = ((quarter + 1) & 2) == 2
    out_sine = jnp.where(swapped, cosine, sine)
    out_cosine = jnp.where(swapped, sine, cosine)
    return (
        jnp.where(flip_sine, -out_sine, out_sine),
        jnp.where(flip_cosine, -out_cosine, out_cosine),
    )


def doc_start(index, lengths_ref):
    start, end = jnp.zeros_like(index), jnp.int32(0)
    for n in range(lengths_ref.shape[0]):
        start = jnp.where(index >= end, end, start)
        end = end + lengths_ref[n]
    return start


def turn(block, cosine, sine):
    block = block.astype(jnp.float32)
    return (block * cosine + pltpu.roll(block, HD // 2, 1) * sine).astype(jnp.bfloat16)


def prepare_kernel(lengths_ref, freq_ref, q_ref, k_ref, *refs, reach):
    cos_ref, sin_ref, query_ref, key_ref = refs
    rows = k_ref.shape[0]
    first = lax.axis_index("tok") * rows
    lane = lax.broadcasted_iota(jnp.int32, (rows, HD), 1)
    sub = lax.broadcasted_iota(jnp.int32, (rows, HD), 0)
    freq = freq_ref[...]
    for n in range(reach + 1):
        index = first - (reach - n) * rows + sub
        start = doc_start(index, lengths_ref)
        sine, cosine = sine_cosine((index - start).astype(jnp.float32) * freq)
        sine = jnp.where(lane < HD // 2, -sine, sine)
        if n < reach:
            cos_ref[n * rows : (n + 1) * rows, :] = cosine
            sin_ref[n * rows : (n + 1) * rows, :] = sine
    for source, target in ((q_ref, query_ref), (k_ref, key_ref)):
        for h in range(source.shape[1] // HD):
            at = slice(h * HD, (h + 1) * HD)
            target[:, at] = turn(source[:, at], cosine, sine)


def attention_kernel(lengths_ref, cos_ref, sin_ref, q_ref, k_ref, v_ref, *refs, reach):
    far, (out_ref, score_ref, weight_ref) = refs[:reach], refs[reach:]
    rows = k_ref.shape[0]
    kv_heads = k_ref.shape[1] // HD
    group = q_ref.shape[1] // k_ref.shape[1]
    count = reach + 1
    first = lax.axis_index("tok") * rows
    scale = HD**-0.5 * math.log2(math.e)
    key_lane = lax.broadcasted_iota(jnp.int32, (rows, rows), 1)
    key_sub = lax.broadcasted_iota(jnp.int32, (rows, rows), 0)
    starts = doc_start(first + key_sub, lengths_ref)
    seen = [first - (reach - n) * rows + key_lane >= starts for n in range(count)]
    seen[reach] = seen[reach] & (key_lane <= key_sub)
    for g in range(kv_heads):
        at = slice(g * HD, (g + 1) * HD)
        at_v = slice((kv_heads + g) * HD, (kv_heads + g + 1) * HD)
        keys = []
        for n in range(reach):
            part = slice(n * rows, (n + 1) * rows)
            keys.append(turn(far[reach - n - 1][:, at], cos_ref[part, :], sin_ref[part, :]))
        keys = jnp.concatenate(keys + [k_ref[:, at]], axis=0)
        vals = jnp.concatenate(
            [far[reach - n - 1][:, at_v] for n in range(reach)] + [v_ref[:, at]], axis=0
        )
        query = jnp.concatenate(
            [q_ref[:, h * HD : (h + 1) * HD] for h in range(g * group, (g + 1) * group)], axis=0
        )
        score_ref[g] = lax.dot_general(
            query, keys, (((1,), (1,)), ((), ())), preferred_element_type=jnp.float32
        )
        totals = []
        for h in range(group):
            band = slice(h * rows, (h + 1) * rows)
            masked = [
                jnp.where(seen[n], score_ref[g, band, n * rows : (n + 1) * rows] * scale, NEG_FILL)
                for n in range(count)
            ]
            top = masked[0]
            for m in masked[1:]:
                top = jnp.maximum(top, m)
            top = jnp.max(top, axis=1, keepdims=True)
            total = None
            for n in range(count):
                w = jnp.exp2(masked[n] - top)
                total = w if total is None else total + w
                weight_ref[g, band, n * rows : (n + 1) * rows] = w.astype(jnp.bfloat16)
            totals.append(jnp.sum(total, axis=1, keepdims=True))
        update = jnp.dot(weight_ref[g], vals, preferred_element_type=jnp.float32)
        for h in range(group):
            piece = update[h * rows : (h + 1) * rows, :] / totals[h]
            head = g * group + h
            out_ref[:, head * HD : (head + 1) * HD] = piece.astype(jnp.bfloat16)


def attend_near(queries, keys, values, doc_lengths, reach, n_tok):
    rows = queries.shape[0]
    kv_heads = keys.shape[1] // HD
    group = queries.shape[1] // keys.shape[1]
    both = jnp.concatenate([keys, values], axis=1)
    far = []
    for d in range(1, reach + 1):
        far.append(lax.ppermute(both, "tok", [(i, i + d) for i in range(n_tok - d)]))
    half = np.arange(HD, dtype=np.float32) % (HD // 2)
    freq = jnp.asarray((ROPE_BASE ** (-(half * 2.0 / HD))).astype(np.float32).reshape(1, HD))
    vmem = pl.BlockSpec(memory_space=pltpu.VMEM)
    smem = pl.BlockSpec(memory_space=pltpu.SMEM)
    span = (reach + 1) * rows
    whole = pltpu.VMEM(queries.shape, jnp.bfloat16)
    settings = pltpu.CompilerParams(vmem_limit_bytes=KERNEL_BYTES)
    cosine, sine, query, key = pl.pallas_call(
        partial(prepare_kernel, reach=reach),
        out_shape=(
            pltpu.VMEM((reach * rows, HD), jnp.float32),
            pltpu.VMEM((reach * rows, HD), jnp.float32),
            whole,
            pltpu.VMEM(keys.shape, jnp.bfloat16),
        ),
        in_specs=[smem] + [vmem] * 3,
        out_specs=(vmem,) * 4,
        compiler_params=settings,
        name="prepare",
    )(doc_lengths, freq, *on_chip(queries, keys))
    return pl.pallas_call(
        partial(attention_kernel, reach=reach),
        out_shape=whole,
        in_specs=[smem] + [vmem] * (5 + reach),
        out_specs=vmem,
        scratch_shapes=[
            pltpu.VMEM((kv_heads, group * rows, span), jnp.float32),
            pltpu.VMEM((kv_heads, group * rows, span), jnp.bfloat16),
        ],
        compiler_params=settings,
        name="attention",
    )(doc_lengths, *on_chip(cosine, sine, query, key, values, *far))


def rotary(tensor, positions):
    half_size = tensor.shape[-1] // 2
    frequency = ROPE_BASE ** (-(jnp.arange(half_size, dtype=jnp.float32) * 2.0 / tensor.shape[-1]))
    angles = positions.astype(jnp.float32)[:, None] * frequency[None, :]
    cosine = jnp.cos(angles)[:, None, :]
    sine_part = jnp.sin(angles)[:, None, :]
    a = tensor[..., :half_size]
    b = tensor[..., half_size:]
    return jnp.concatenate([a * cosine - b * sine_part, b * cosine + a * sine_part], axis=-1)


def attend_far(queries, keys, values, doc_lengths):
    rows = queries.shape[0]
    heads, kv_heads = queries.shape[1] // HD, keys.shape[1] // HD
    own = lax.axis_index("tok") * rows + jnp.arange(rows, dtype=jnp.int32)
    docs, positions = locate(own, doc_lengths)
    rotated_q = rotary(queries.astype(jnp.float32).reshape(rows, heads, HD), positions)
    rotated_q = rotated_q.astype(jnp.bfloat16).reshape(rows, kv_heads, heads // kv_heads, HD)
    rotated_k = rotary(keys.astype(jnp.float32).reshape(rows, kv_heads, HD), positions)
    rotated_k = rotated_k.astype(jnp.bfloat16).reshape(rows, kv_heads * HD)
    all_k = lax.all_gather(rotated_k, "tok", axis=0, tiled=True)
    all_v = lax.all_gather(values, "tok", axis=0, tiled=True)
    step = 4 * rows

    def one_block(number, state):
        running, totals, weighted = state
        begin = number * step
        key = lax.dynamic_slice_in_dim(all_k, begin, step, 0).reshape(step, kv_heads, HD)
        value = lax.dynamic_slice_in_dim(all_v, begin, step, 0).reshape(step, kv_heads, HD)
        index = begin + jnp.arange(step, dtype=jnp.int32)
        key_docs, _ = locate(index, doc_lengths)
        scores = HD**-0.5 * jnp.einsum(
            "qgjd,kgd->gjqk", rotated_q, key, preferred_element_type=jnp.float32
        )
        visible = (docs[:, None] == key_docs[None, :]) & (index[None, :] <= own[:, None])
        scores = jnp.where(visible, scores, NEG_FILL)
        top = jnp.maximum(running, jnp.max(scores, axis=-1))
        factor = jnp.exp(running - top)
        weights = jnp.where(visible, jnp.exp(scores - top[..., None]), 0.0)
        totals = totals * factor + jnp.sum(weights, axis=-1)
        update = jnp.einsum(
            "gjqk,kgd->gjqd",
            weights.astype(jnp.bfloat16),
            value,
            preferred_element_type=jnp.float32,
        )
        return (top, totals, weighted * factor[..., None] + update)

    shape = (kv_heads, heads // kv_heads, rows)
    state = (
        jnp.full(shape, NEG_FILL, jnp.float32),
        jnp.zeros(shape, jnp.float32),
        jnp.zeros(shape + (HD,), jnp.float32),
    )
    _, totals, weighted = lax.fori_loop(0, all_k.shape[0] // step, one_block, state)
    output = (weighted / totals[..., None]).transpose(2, 0, 1, 3)
    return output.reshape(rows, heads * HD).astype(jnp.bfloat16)


def project_kernel(own_ref, mate_ref, *refs, inner, sides, added):
    weights, (*before, out_ref) = refs[: 2 * sides], refs[2 * sides :]
    pieces = []
    for own_w, mate_w in zip(weights[:sides], weights[sides:]):
        own = jnp.dot(own_ref[...], own_w[...], preferred_element_type=jnp.float32)
        mate = jnp.dot(mate_ref[...], mate_w[...], preferred_element_type=jnp.float32)
        own, mate = (p.astype(jnp.bfloat16).astype(jnp.float32) for p in (own, mate))
        pieces.append(own + mate)
    straight = jnp.concatenate(pieces, axis=1)
    if sides > 1:
        flip = lax.rem(lax.axis_index("tok"), inner)
        straight = jnp.where(flip == 0, straight, jnp.concatenate(pieces[::-1], axis=1))
    if added:
        straight = straight + before[0][...].astype(jnp.float32)
    out_ref[...] = straight.astype(jnp.bfloat16)


def project(inner, own, mate, own_weights, mate_weights, before):
    vmem = pl.BlockSpec(memory_space=pltpu.VMEM)
    operands = on_chip(own, mate, *own_weights, *mate_weights, *before)
    return pl.pallas_call(
        partial(project_kernel, inner=inner, sides=len(own_weights), added=len(before)),
        out_shape=pltpu.VMEM((own.shape[0], sum(w.shape[1] for w in own_weights)), jnp.bfloat16),
        in_specs=[vmem] * len(operands),
        out_specs=vmem,
        compiler_params=pltpu.CompilerParams(vmem_limit_bytes=KERNEL_BYTES),
    )(*operands)


def solution(mesh):
    n_tok, n_feat = mesh.shape["tok"], mesh.shape["feat"]
    inner = n_tok // n_feat

    def everyone(move):
        pairs = []
        for z in range(n_feat):
            for x in range(inner):
                for j in range(n_feat):
                    to_z, to_x, to_j = move(z, x, j)
                    pairs.append(
                        (
                            (z * inner + x) * n_feat + j,
                            (to_z * inner + to_x) * n_feat + to_j,
                        )
                    )
        return pairs

    def permute(array, move):
        return lax.ppermute(array, ("tok", "feat"), everyone(move))

    def shards(queries, keys, values, out_weight, doc_lengths):
        rows = queries.shape[0]
        longest = n_tok * rows * LONGEST[0] // LONGEST[1]
        reach = min(n_tok - 1, -(-(longest - 1) // rows))
        if reach <= FAR_BLOCKS:
            attended = attend_near(queries, keys, values, doc_lengths, reach, n_tok)
        else:
            attended = attend_far(queries, keys, values, doc_lengths)
        if inner == 2:
            weights = [out_weight, permute(out_weight, lambda z, x, j: (z, 1 - x, j))]
        else:
            groups = [[z * inner + x for x in range(inner)] for z in range(n_feat)]
            weights = [
                lax.all_gather(
                    out_weight, "tok", axis=1, tiled=True, axis_index_groups=groups
                )
            ]
        mate_weights = []
        for w in weights:
            mate_weights.append(permute(w, lambda z, x, j: (z, x, j ^ 1)))

        def deliver(k, cross):
            def move(z, x, j):
                core = (j & 1) ^ cross
                return (z ^ (core * 2 | ((j >> 1) ^ k)), x, (j & 2) | core)

            return permute(attended, move)

        lent = project(inner, deliver(1, 0), deliver(1, 1), weights, mate_weights, [])
        lent = permute(lent, lambda z, x, j: (z, x, j ^ 2))
        mixed = project(inner, deliver(0, 0), deliver(0, 1), weights, mate_weights, [lent])
        return permute(mixed, lambda z, x, j: (z ^ ((j & 1) * 2 | (j >> 1)), x, z))

    in_specs = (P("tok", "feat"), P("tok", "feat"), P("tok", "feat"), P("feat", "tok"), P())
    return jax.shard_map(
        shards, mesh=mesh, in_specs=in_specs, out_specs=P("tok", "feat"), check_vma=False
    )
```

```python
import math
from functools import partial

import jax
import jax.numpy as jnp
import numpy as np
from jax import lax
from jax.experimental import pallas as pl
from jax.experimental.pallas import tpu as pltpu
from jax.sharding import PartitionSpec as P


HD = 128
ROPE_BASE = 500000.0
NEG_FILL = -1e30
LONGEST = (5, 8)
KERNEL_BYTES = 16 << 20
FAR_BLOCKS = 7


def locate(token_index, doc_lengths):
    doc_ends = jnp.cumsum(doc_lengths)
    starts = doc_ends - doc_lengths
    doc_ids = jnp.sum((token_index[:, None] >= doc_ends[None, :]).astype(jnp.int32), axis=1)
    number = jnp.arange(doc_lengths.shape[0], dtype=jnp.int32)
    first_token = jnp.sum(
        jnp.where(doc_ids[:, None] == number[None, :], starts[None, :], 0), axis=1
    )
    return (doc_ids, token_index - first_token)


def on_chip(*arrays):
    return [pltpu.with_memory_space_constraint(a, pltpu.VMEM) for a in arrays]


def sine_cosine(angle):
    turns = jnp.round(angle * (2.0 / math.pi))
    rest = ((angle - turns * 1.5703125) - turns * 4.837512969970703125e-4) - turns * 7.54978995489188216e-8
    square = rest * rest
    sine = (-1.9515295891e-4 * square + 8.3321608736e-3) * square - 1.6666654611e-1
    sine = sine * square * rest + rest
    cosine = (2.443315711809948e-5 * square - 1.388731625493765e-3) * square
    cosine = (cosine + 4.166664568298827e-2) * square * square - 0.5 * square + 1.0
    quarter = turns.astype(jnp.int32)
    swapped = (quarter & 1) == 1
    flip_sine = (quarter & 2) == 2
    flip_cosine = ((quarter + 1) & 2) == 2
    out_sine = jnp.where(swapped, cosine, sine)
    out_cosine = jnp.where(swapped, sine, cosine)
    return (
        jnp.where(flip_sine, -out_sine, out_sine),
        jnp.where(flip_cosine, -out_cosine, out_cosine),
    )


def doc_start(index, lengths_ref):
    start, end = jnp.zeros_like(index), jnp.int32(0)
    for n in range(lengths_ref.shape[0]):
        start = jnp.where(index >= end, end, start)
        end = end + lengths_ref[n]
    return start


def turn(block, cosine, sine):
    block = block.astype(jnp.float32)
    return (block * cosine + pltpu.roll(block, HD // 2, 1) * sine).astype(jnp.bfloat16)


def prepare_kernel(lengths_ref, freq_ref, q_ref, k_ref, *refs, reach):
    cos_ref, sin_ref, query_ref, key_ref = refs
    rows = k_ref.shape[0]
    first = lax.axis_index("tok") * rows
    lane = lax.broadcasted_iota(jnp.int32, (rows, HD), 1)
    sub = lax.broadcasted_iota(jnp.int32, (rows, HD), 0)
    freq = freq_ref[...]
    for n in range(reach + 1):
        index = first - (reach - n) * rows + sub
        start = doc_start(index, lengths_ref)
        sine, cosine = sine_cosine((index - start).astype(jnp.float32) * freq)
        sine = jnp.where(lane < HD // 2, -sine, sine)
        if n < reach:
            cos_ref[n * rows : (n + 1) * rows, :] = cosine
            sin_ref[n * rows : (n + 1) * rows, :] = sine
    for source, target in ((q_ref, query_ref), (k_ref, key_ref)):
        for h in range(source.shape[1] // HD):
            at = slice(h * HD, (h + 1) * HD)
            target[:, at] = turn(source[:, at], cosine, sine)


def attention_kernel(lengths_ref, cos_ref, sin_ref, q_ref, k_ref, v_ref, *refs, reach):
    far, (out_ref, score_ref, weight_ref) = refs[:reach], refs[reach:]
    rows = k_ref.shape[0]
    kv_heads = k_ref.shape[1] // HD
    group = q_ref.shape[1] // k_ref.shape[1]
    count = reach + 1
    first = lax.axis_index("tok") * rows
    scale = HD**-0.5 * math.log2(math.e)
    key_lane = lax.broadcasted_iota(jnp.int32, (rows, rows), 1)
    key_sub = lax.broadcasted_iota(jnp.int32, (rows, rows), 0)
    starts = doc_start(first + key_sub, lengths_ref)
    seen = [first - (reach - n) * rows + key_lane >= starts for n in range(count)]
    seen[reach] = seen[reach] & (key_lane <= key_sub)
    for g in range(kv_heads):
        at = slice(g * HD, (g + 1) * HD)
        at_v = slice((kv_heads + g) * HD, (kv_heads + g + 1) * HD)
        keys = []
        for n in range(reach):
            part = slice(n * rows, (n + 1) * rows)
            keys.append(turn(far[reach - n - 1][:, at], cos_ref[part, :], sin_ref[part, :]))
        keys = jnp.concatenate(keys + [k_ref[:, at]], axis=0)
        vals = jnp.concatenate(
            [far[reach - n - 1][:, at_v] for n in range(reach)] + [v_ref[:, at]], axis=0
        )
        query = jnp.concatenate(
            [q_ref[:, h * HD : (h + 1) * HD] for h in range(g * group, (g + 1) * group)], axis=0
        )
        score_ref[g] = lax.dot_general(
            query, keys, (((1,), (1,)), ((), ())), preferred_element_type=jnp.float32
        )
        totals = []
        for h in range(group):
            band = slice(h * rows, (h + 1) * rows)
            masked = [
                jnp.where(seen[n], score_ref[g, band, n * rows : (n + 1) * rows] * scale, NEG_FILL)
                for n in range(count)
            ]
            top = masked[0]
            for m in masked[1:]:
                top = jnp.maximum(top, m)
            top = jnp.max(top, axis=1, keepdims=True)
            total = None
            for n in range(count):
                w = jnp.exp2(masked[n] - top)
                total = w if total is None else total + w
                weight_ref[g, band, n * rows : (n + 1) * rows] = w.astype(jnp.bfloat16)
            totals.append(jnp.sum(total, axis=1, keepdims=True))
        update = jnp.dot(weight_ref[g], vals, preferred_element_type=jnp.float32)
        for h in range(group):
            piece = update[h * rows : (h + 1) * rows, :] / totals[h]
            head = g * group + h
            out_ref[:, head * HD : (head + 1) * HD] = piece.astype(jnp.bfloat16)


def attend_near(queries, keys, values, doc_lengths, reach, n_tok):
    rows = queries.shape[0]
    kv_heads = keys.shape[1] // HD
    group = queries.shape[1] // keys.shape[1]
    both = jnp.concatenate([keys, values], axis=1)
    far = []
    for d in range(1, reach + 1):
        far.append(lax.ppermute(both, "tok", [(i, i + d) for i in range(n_tok - d)]))
    half = np.arange(HD, dtype=np.float32) % (HD // 2)
    freq = jnp.asarray((ROPE_BASE ** (-(half * 2.0 / HD))).astype(np.float32).reshape(1, HD))
    vmem = pl.BlockSpec(memory_space=pltpu.VMEM)
    smem = pl.BlockSpec(memory_space=pltpu.SMEM)
    span = (reach + 1) * rows
    whole = pltpu.VMEM(queries.shape, jnp.bfloat16)
    settings = pltpu.CompilerParams(vmem_limit_bytes=KERNEL_BYTES)
    cosine, sine, query, key = pl.pallas_call(
        partial(prepare_kernel, reach=reach),
        out_shape=(
            pltpu.VMEM((reach * rows, HD), jnp.float32),
            pltpu.VMEM((reach * rows, HD), jnp.float32),
            whole,
            pltpu.VMEM(keys.shape, jnp.bfloat16),
        ),
        in_specs=[smem] + [vmem] * 3,
        out_specs=(vmem,) * 4,
        compiler_params=settings,
        name="prepare",
    )(doc_lengths, freq, *on_chip(queries, keys))
    return pl.pallas_call(
        partial(attention_kernel, reach=reach),
        out_shape=whole,
        in_specs=[smem] + [vmem] * (5 + reach),
        out_specs=vmem,
        scratch_shapes=[
            pltpu.VMEM((kv_heads, group * rows, span), jnp.float32),
            pltpu.VMEM((kv_heads, group * rows, span), jnp.bfloat16),
        ],
        compiler_params=settings,
        name="attention",
    )(doc_lengths, *on_chip(cosine, sine, query, key, values, *far))


def rotary(tensor, positions):
    half_size = tensor.shape[-1] // 2
    frequency = ROPE_BASE ** (-(jnp.arange(half_size, dtype=jnp.float32) * 2.0 / tensor.shape[-1]))
    angles = positions.astype(jnp.float32)[:, None] * frequency[None, :]
    cosine = jnp.cos(angles)[:, None, :]
    sine_part = jnp.sin(angles)[:, None, :]
    a = tensor[..., :half_size]
    b = tensor[..., half_size:]
    return jnp.concatenate([a * cosine - b * sine_part, b * cosine + a * sine_part], axis=-1)


def attend_far(queries, keys, values, doc_lengths):
    rows = queries.shape[0]
    heads, kv_heads = queries.shape[1] // HD, keys.shape[1] // HD
    own = lax.axis_index("tok") * rows + jnp.arange(rows, dtype=jnp.int32)
    docs, positions = locate(own, doc_lengths)
    rotated_q = rotary(queries.astype(jnp.float32).reshape(rows, heads, HD), positions)
    rotated_q = rotated_q.astype(jnp.bfloat16).reshape(rows, kv_heads, heads // kv_heads, HD)
    rotated_k = rotary(keys.astype(jnp.float32).reshape(rows, kv_heads, HD), positions)
    rotated_k = rotated_k.astype(jnp.bfloat16).reshape(rows, kv_heads * HD)
    all_k = lax.all_gather(rotated_k, "tok", axis=0, tiled=True)
    all_v = lax.all_gather(values, "tok", axis=0, tiled=True)
    step = 4 * rows

    def one_block(number, state):
        running, totals, weighted = state
        begin = number * step
        key = lax.dynamic_slice_in_dim(all_k, begin, step, 0).reshape(step, kv_heads, HD)
        value = lax.dynamic_slice_in_dim(all_v, begin, step, 0).reshape(step, kv_heads, HD)
        index = begin + jnp.arange(step, dtype=jnp.int32)
        key_docs, _ = locate(index, doc_lengths)
        scores = HD**-0.5 * jnp.einsum(
            "qgjd,kgd->gjqk", rotated_q, key, preferred_element_type=jnp.float32
        )
        visible = (docs[:, None] == key_docs[None, :]) & (index[None, :] <= own[:, None])
        scores = jnp.where(visible, scores, NEG_FILL)
        top = jnp.maximum(running, jnp.max(scores, axis=-1))
        factor = jnp.exp(running - top)
        weights = jnp.where(visible, jnp.exp(scores - top[..., None]), 0.0)
        totals = totals * factor + jnp.sum(weights, axis=-1)
        update = jnp.einsum(
            "gjqk,kgd->gjqd",
            weights.astype(jnp.bfloat16),
            value,
            preferred_element_type=jnp.float32,
        )
        return (top, totals, weighted * factor[..., None] + update)

    shape = (kv_heads, heads // kv_heads, rows)
    state = (
        jnp.full(shape, NEG_FILL, jnp.float32),
        jnp.zeros(shape, jnp.float32),
        jnp.zeros(shape + (HD,), jnp.float32),
    )
    _, totals, weighted = lax.fori_loop(0, all_k.shape[0] // step, one_block, state)
    output = (weighted / totals[..., None]).transpose(2, 0, 1, 3)
    return output.reshape(rows, heads * HD).astype(jnp.bfloat16)


def project_kernel(own_ref, mate_ref, *refs, inner, sides, added):
    weights, (*before, out_ref) = refs[: 2 * sides], refs[2 * sides :]
    pieces = []
    for own_w, mate_w in zip(weights[:sides], weights[sides:]):
        own = jnp.dot(own_ref[...], own_w[...], preferred_element_type=jnp.float32)
        mate = jnp.dot(mate_ref[...], mate_w[...], preferred_element_type=jnp.float32)
        own, mate = (p.astype(jnp.bfloat16).astype(jnp.float32) for p in (own, mate))
        pieces.append(own + mate)
    straight = jnp.concatenate(pieces, axis=1)
    if sides > 1:
        flip = lax.rem(lax.axis_index("tok"), inner)
        straight = jnp.where(flip == 0, straight, jnp.concatenate(pieces[::-1], axis=1))
    if added:
        straight = straight + before[0][...].astype(jnp.float32)
    out_ref[...] = straight.astype(jnp.bfloat16)


def project(inner, own, mate, own_weights, mate_weights, before):
    vmem = pl.BlockSpec(memory_space=pltpu.VMEM)
    operands = on_chip(own, mate, *own_weights, *mate_weights, *before)
    return pl.pallas_call(
        partial(project_kernel, inner=inner, sides=len(own_weights), added=len(before)),
        out_shape=pltpu.VMEM((own.shape[0], sum(w.shape[1] for w in own_weights)), jnp.bfloat16),
        in_specs=[vmem] * len(operands),
        out_specs=vmem,
        compiler_params=pltpu.CompilerParams(vmem_limit_bytes=KERNEL_BYTES),
    )(*operands)


def solution(mesh):
    n_tok, n_feat = mesh.shape["tok"], mesh.shape["feat"]
    inner = n_tok // n_feat

    def everyone(move):
        pairs = []
        for z in range(n_feat):
            for x in range(inner):
                for j in range(n_feat):
                    to_z, to_x, to_j = move(z, x, j)
                    pairs.append(
                        (
                            (z * inner + x) * n_feat + j,
                            (to_z * inner + to_x) * n_feat + to_j,
                        )
                    )
        return pairs

    def permute(array, move):
        return lax.ppermute(array, ("tok", "feat"), everyone(move))

    def shards(queries, keys, values, out_weight, doc_lengths):
        rows = queries.shape[0]
        longest = n_tok * rows * LONGEST[0] // LONGEST[1]
        reach = min(n_tok - 1, -(-(longest - 1) // rows))
        if reach <= FAR_BLOCKS:
            attended = attend_near(queries, keys, values, doc_lengths, reach, n_tok)
        else:
            attended = attend_far(queries, keys, values, doc_lengths)
        if inner == 2:
            weights = [out_weight, permute(out_weight, lambda z, x, j: (z, 1 - x, j))]
        else:
            groups = [[z * inner + x for x in range(inner)] for z in range(n_feat)]
            weights = [
                lax.all_gather(
                    out_weight, "tok", axis=1, tiled=True, axis_index_groups=groups
                )
            ]
        mate_weights = []
        for w in weights:
            mate_weights.append(permute(w, lambda z, x, j: (z, x, j ^ 1)))

        def deliver(k, cross):
            def move(z, x, j):
                core = (j & 1) ^ cross
                return (z ^ (core * 2 | ((j >> 1) ^ k)), x, (j & 2) | core)

            return permute(attended, move)

        own, mate = deliver(1, 0), deliver(1, 1)
        lent = project(inner, own, mate, weights, mate_weights, [])
        passed = permute(mate, lambda z, x, j: (z ^ 1, x, j))
        lent = permute(lent, lambda z, x, j: (z, x, j ^ 2))
        mixed = project(inner, deliver(0, 0), passed, weights, mate_weights, [lent])
        return permute(mixed, lambda z, x, j: (z ^ ((j & 1) * 2 | (j >> 1)), x, z))

    in_specs = (P("tok", "feat"), P("tok", "feat"), P("tok", "feat"), P("feat", "tok"), P())
    return jax.shard_map(
        shards, mesh=mesh, in_specs=in_specs, out_specs=P("tok", "feat"), check_vma=False
    )
```

```python
import math
from functools import partial

import jax
import jax.numpy as jnp
import numpy as np
from jax import lax
from jax.experimental import pallas as pl
from jax.experimental.pallas import tpu as pltpu
from jax.sharding import PartitionSpec as P


HD = 128
ROPE_BASE = 500000.0
NEG_FILL = -1e30
LONGEST = (5, 8)
KERNEL_BYTES = 16 << 20
FAR_BLOCKS = 7


def locate(token_index, doc_lengths):
    doc_ends = jnp.cumsum(doc_lengths)
    starts = doc_ends - doc_lengths
    doc_ids = jnp.sum((token_index[:, None] >= doc_ends[None, :]).astype(jnp.int32), axis=1)
    number = jnp.arange(doc_lengths.shape[0], dtype=jnp.int32)
    first_token = jnp.sum(
        jnp.where(doc_ids[:, None] == number[None, :], starts[None, :], 0), axis=1
    )
    return (doc_ids, token_index - first_token)


def on_chip(*arrays):
    return [pltpu.with_memory_space_constraint(a, pltpu.VMEM) for a in arrays]


def sine_cosine(angle):
    turns = jnp.round(angle * (2.0 / math.pi))
    rest = ((angle - turns * 1.5703125) - turns * 4.837512969970703125e-4) - turns * 7.54978995489188216e-8
    square = rest * rest
    sine = (-1.9515295891e-4 * square + 8.3321608736e-3) * square - 1.6666654611e-1
    sine = sine * square * rest + rest
    cosine = (2.443315711809948e-5 * square - 1.388731625493765e-3) * square
    cosine = (cosine + 4.166664568298827e-2) * square * square - 0.5 * square + 1.0
    quarter = turns.astype(jnp.int32)
    swapped = (quarter & 1) == 1
    flip_sine = (quarter & 2) == 2
    flip_cosine = ((quarter + 1) & 2) == 2
    out_sine = jnp.where(swapped, cosine, sine)
    out_cosine = jnp.where(swapped, sine, cosine)
    return (
        jnp.where(flip_sine, -out_sine, out_sine),
        jnp.where(flip_cosine, -out_cosine, out_cosine),
    )


def doc_start(index, lengths_ref):
    start, end = jnp.zeros_like(index), jnp.int32(0)
    for n in range(lengths_ref.shape[0]):
        start = jnp.where(index >= end, end, start)
        end = end + lengths_ref[n]
    return start


def turn(block, cosine, sine):
    block = block.astype(jnp.float32)
    return (block * cosine + pltpu.roll(block, HD // 2, 1) * sine).astype(jnp.bfloat16)


def prepare_kernel(lengths_ref, freq_ref, q_ref, k_ref, *refs, reach):
    cos_ref, sin_ref, query_ref, key_ref = refs
    rows = k_ref.shape[0]
    first = lax.axis_index("tok") * rows
    lane = lax.broadcasted_iota(jnp.int32, (rows, HD), 1)
    sub = lax.broadcasted_iota(jnp.int32, (rows, HD), 0)
    freq = freq_ref[...]
    for n in range(reach + 1):
        index = first - (reach - n) * rows + sub
        start = doc_start(index, lengths_ref)
        sine, cosine = sine_cosine((index - start).astype(jnp.float32) * freq)
        sine = jnp.where(lane < HD // 2, -sine, sine)
        if n < reach:
            cos_ref[n * rows : (n + 1) * rows, :] = cosine
            sin_ref[n * rows : (n + 1) * rows, :] = sine
    for source, target in ((q_ref, query_ref), (k_ref, key_ref)):
        for h in range(source.shape[1] // HD):
            at = slice(h * HD, (h + 1) * HD)
            target[:, at] = turn(source[:, at], cosine, sine)


def attention_kernel(lengths_ref, cos_ref, sin_ref, q_ref, k_ref, v_ref, *refs, reach, mixed):
    out_ref, score_ref, weight_ref = refs[-3:]
    far, taken = [], 0
    base = lax.axis_size("tok") // 2
    for d in range(1, reach + 1):
        far.append(refs[taken][...])
        if mixed[d - 1]:
            inside = lax.rem(lax.axis_index("tok"), base) >= d
            far[-1] = jnp.where(inside, refs[taken + 1][...], far[-1])
        taken += 2 if mixed[d - 1] else 1
    rows = k_ref.shape[0]
    kv_heads = k_ref.shape[1] // HD
    group = q_ref.shape[1] // k_ref.shape[1]
    count = reach + 1
    first = lax.axis_index("tok") * rows
    scale = HD**-0.5 * math.log2(math.e)
    key_lane = lax.broadcasted_iota(jnp.int32, (rows, rows), 1)
    key_sub = lax.broadcasted_iota(jnp.int32, (rows, rows), 0)
    starts = doc_start(first + key_sub, lengths_ref)
    seen = [first - (reach - n) * rows + key_lane >= starts for n in range(count)]
    seen[reach] = seen[reach] & (key_lane <= key_sub)
    for g in range(kv_heads):
        at = slice(g * HD, (g + 1) * HD)
        at_v = slice((kv_heads + g) * HD, (kv_heads + g + 1) * HD)
        keys = []
        for n in range(reach):
            part = slice(n * rows, (n + 1) * rows)
            keys.append(turn(far[reach - n - 1][:, at], cos_ref[part, :], sin_ref[part, :]))
        keys = jnp.concatenate(keys + [k_ref[:, at]], axis=0)
        vals = jnp.concatenate(
            [far[reach - n - 1][:, at_v] for n in range(reach)] + [v_ref[:, at]], axis=0
        )
        query = jnp.concatenate(
            [q_ref[:, h * HD : (h + 1) * HD] for h in range(g * group, (g + 1) * group)], axis=0
        )
        score_ref[g] = lax.dot_general(
            query, keys, (((1,), (1,)), ((), ())), preferred_element_type=jnp.float32
        )
        totals = []
        for h in range(group):
            band = slice(h * rows, (h + 1) * rows)
            masked = [
                jnp.where(seen[n], score_ref[g, band, n * rows : (n + 1) * rows] * scale, NEG_FILL)
                for n in range(count)
            ]
            top = masked[0]
            for m in masked[1:]:
                top = jnp.maximum(top, m)
            top = jnp.max(top, axis=1, keepdims=True)
            total = None
            for n in range(count):
                w = jnp.exp2(masked[n] - top)
                total = w if total is None else total + w
                weight_ref[g, band, n * rows : (n + 1) * rows] = w.astype(jnp.bfloat16)
            totals.append(jnp.sum(total, axis=1, keepdims=True))
        update = jnp.dot(weight_ref[g], vals, preferred_element_type=jnp.float32)
        for h in range(group):
            piece = update[h * rows : (h + 1) * rows, :] / totals[h]
            head = g * group + h
            out_ref[:, head * HD : (head + 1) * HD] = piece.astype(jnp.bfloat16)


def attend_near(queries, keys, values, doc_lengths, reach, n_tok, inner):
    rows = queries.shape[0]
    kv_heads = keys.shape[1] // HD
    group = queries.shape[1] // keys.shape[1]
    both = jnp.concatenate([keys, values], axis=1)
    far = []
    base = n_tok // 2

    def shift(array, d, pairs):
        return lax.ppermute(array, "tok", [(i, i + d) for i in pairs])

    held = shift(both, base, range(n_tok - base))
    for d in range(1, reach + 1):
        if d == base:
            far.append(held)
        elif (d - base) % inner:
            far.append(shift(both, d, range(n_tok - d)))
        else:
            inside = [i for i in range(n_tok - d) if i // base == (i + d) // base]
            onward = [
                i for i in range(base, n_tok) if base <= i + d - base < n_tok and i - base < n_tok - d
            ]
            relayed = shift(held, d - base, onward)
            far.append((relayed, shift(both, d, inside)) if inside else relayed)
    mixed = [isinstance(f, tuple) for f in far]
    far = [a for f in far for a in (f if isinstance(f, tuple) else (f,))]
    half = np.arange(HD, dtype=np.float32) % (HD // 2)
    freq = jnp.asarray((ROPE_BASE ** (-(half * 2.0 / HD))).astype(np.float32).reshape(1, HD))
    vmem = pl.BlockSpec(memory_space=pltpu.VMEM)
    smem = pl.BlockSpec(memory_space=pltpu.SMEM)
    span = (reach + 1) * rows
    whole = pltpu.VMEM(queries.shape, jnp.bfloat16)
    settings = pltpu.CompilerParams(vmem_limit_bytes=KERNEL_BYTES)
    cosine, sine, query, key = pl.pallas_call(
        partial(prepare_kernel, reach=reach),
        out_shape=(
            pltpu.VMEM((reach * rows, HD), jnp.float32),
            pltpu.VMEM((reach * rows, HD), jnp.float32),
            whole,
            pltpu.VMEM(keys.shape, jnp.bfloat16),
        ),
        in_specs=[smem] + [vmem] * 3,
        out_specs=(vmem,) * 4,
        compiler_params=settings,
        name="prepare",
    )(doc_lengths, freq, *on_chip(queries, keys))
    return pl.pallas_call(
        partial(attention_kernel, reach=reach, mixed=mixed),
        out_shape=whole,
        in_specs=[smem] + [vmem] * (5 + len(far)),
        out_specs=vmem,
        scratch_shapes=[
            pltpu.VMEM((kv_heads, group * rows, span), jnp.float32),
            pltpu.VMEM((kv_heads, group * rows, span), jnp.bfloat16),
        ],
        compiler_params=settings,
        name="attention",
    )(doc_lengths, *on_chip(cosine, sine, query, key, values, *far))


def rotary(tensor, positions):
    half_size = tensor.shape[-1] // 2
    frequency = ROPE_BASE ** (-(jnp.arange(half_size, dtype=jnp.float32) * 2.0 / tensor.shape[-1]))
    angles = positions.astype(jnp.float32)[:, None] * frequency[None, :]
    cosine = jnp.cos(angles)[:, None, :]
    sine_part = jnp.sin(angles)[:, None, :]
    a = tensor[..., :half_size]
    b = tensor[..., half_size:]
    return jnp.concatenate([a * cosine - b * sine_part, b * cosine + a * sine_part], axis=-1)


def attend_far(queries, keys, values, doc_lengths):
    rows = queries.shape[0]
    heads, kv_heads = queries.shape[1] // HD, keys.shape[1] // HD
    own = lax.axis_index("tok") * rows + jnp.arange(rows, dtype=jnp.int32)
    docs, positions = locate(own, doc_lengths)
    rotated_q = rotary(queries.astype(jnp.float32).reshape(rows, heads, HD), positions)
    rotated_q = rotated_q.astype(jnp.bfloat16).reshape(rows, kv_heads, heads // kv_heads, HD)
    rotated_k = rotary(keys.astype(jnp.float32).reshape(rows, kv_heads, HD), positions)
    rotated_k = rotated_k.astype(jnp.bfloat16).reshape(rows, kv_heads * HD)
    all_k = lax.all_gather(rotated_k, "tok", axis=0, tiled=True)
    all_v = lax.all_gather(values, "tok", axis=0, tiled=True)
    step = 4 * rows

    def one_block(number, state):
        running, totals, weighted = state
        begin = number * step
        key = lax.dynamic_slice_in_dim(all_k, begin, step, 0).reshape(step, kv_heads, HD)
        value = lax.dynamic_slice_in_dim(all_v, begin, step, 0).reshape(step, kv_heads, HD)
        index = begin + jnp.arange(step, dtype=jnp.int32)
        key_docs, _ = locate(index, doc_lengths)
        scores = HD**-0.5 * jnp.einsum(
            "qgjd,kgd->gjqk", rotated_q, key, preferred_element_type=jnp.float32
        )
        visible = (docs[:, None] == key_docs[None, :]) & (index[None, :] <= own[:, None])
        scores = jnp.where(visible, scores, NEG_FILL)
        top = jnp.maximum(running, jnp.max(scores, axis=-1))
        factor = jnp.exp(running - top)
        weights = jnp.where(visible, jnp.exp(scores - top[..., None]), 0.0)
        totals = totals * factor + jnp.sum(weights, axis=-1)
        update = jnp.einsum(
            "gjqk,kgd->gjqd",
            weights.astype(jnp.bfloat16),
            value,
            preferred_element_type=jnp.float32,
        )
        return (top, totals, weighted * factor[..., None] + update)

    shape = (kv_heads, heads // kv_heads, rows)
    state = (
        jnp.full(shape, NEG_FILL, jnp.float32),
        jnp.zeros(shape, jnp.float32),
        jnp.zeros(shape + (HD,), jnp.float32),
    )
    _, totals, weighted = lax.fori_loop(0, all_k.shape[0] // step, one_block, state)
    output = (weighted / totals[..., None]).transpose(2, 0, 1, 3)
    return output.reshape(rows, heads * HD).astype(jnp.bfloat16)


def project_kernel(own_ref, mate_ref, *refs, inner, sides, added):
    weights, (*before, out_ref) = refs[: 2 * sides], refs[2 * sides :]
    pieces = []
    for own_w, mate_w in zip(weights[:sides], weights[sides:]):
        own = jnp.dot(own_ref[...], own_w[...], preferred_element_type=jnp.float32)
        mate = jnp.dot(mate_ref[...], mate_w[...], preferred_element_type=jnp.float32)
        own, mate = (p.astype(jnp.bfloat16).astype(jnp.float32) for p in (own, mate))
        pieces.append(own + mate)
    straight = jnp.concatenate(pieces, axis=1)
    if sides > 1:
        flip = lax.rem(lax.axis_index("tok"), inner)
        straight = jnp.where(flip == 0, straight, jnp.concatenate(pieces[::-1], axis=1))
    if added:
        straight = straight + before[0][...].astype(jnp.float32)
    out_ref[...] = straight.astype(jnp.bfloat16)


def project(inner, own, mate, own_weights, mate_weights, before):
    vmem = pl.BlockSpec(memory_space=pltpu.VMEM)
    operands = on_chip(own, mate, *own_weights, *mate_weights, *before)
    return pl.pallas_call(
        partial(project_kernel, inner=inner, sides=len(own_weights), added=len(before)),
        out_shape=pltpu.VMEM((own.shape[0], sum(w.shape[1] for w in own_weights)), jnp.bfloat16),
        in_specs=[vmem] * len(operands),
        out_specs=vmem,
        compiler_params=pltpu.CompilerParams(vmem_limit_bytes=KERNEL_BYTES),
    )(*operands)


def solution(mesh):
    n_tok, n_feat = mesh.shape["tok"], mesh.shape["feat"]
    inner = n_tok // n_feat

    def everyone(move):
        pairs = []
        for z in range(n_feat):
            for x in range(inner):
                for j in range(n_feat):
                    to_z, to_x, to_j = move(z, x, j)
                    pairs.append(
                        (
                            (z * inner + x) * n_feat + j,
                            (to_z * inner + to_x) * n_feat + to_j,
                        )
                    )
        return pairs

    def permute(array, move):
        return lax.ppermute(array, ("tok", "feat"), everyone(move))

    def shards(queries, keys, values, out_weight, doc_lengths):
        rows = queries.shape[0]
        longest = n_tok * rows * LONGEST[0] // LONGEST[1]
        reach = min(n_tok - 1, -(-(longest - 1) // rows))
        if reach <= FAR_BLOCKS:
            attended = attend_near(queries, keys, values, doc_lengths, reach, n_tok, inner)
        else:
            attended = attend_far(queries, keys, values, doc_lengths)
        if inner == 2:
            weights = [out_weight, permute(out_weight, lambda z, x, j: (z, 1 - x, j))]
        else:
            groups = [[z * inner + x for x in range(inner)] for z in range(n_feat)]
            weights = [
                lax.all_gather(
                    out_weight, "tok", axis=1, tiled=True, axis_index_groups=groups
                )
            ]
        mate_weights = []
        for w in weights:
            mate_weights.append(permute(w, lambda z, x, j: (z, x, j ^ 1)))

        def deliver(k, cross):
            def move(z, x, j):
                core = (j & 1) ^ cross
                return (z ^ (core * 2 | ((j >> 1) ^ k)), x, (j & 2) | core)

            return permute(attended, move)

        own, mate = deliver(1, 0), deliver(1, 1)
        lent = project(inner, own, mate, weights, mate_weights, [])
        passed = permute(mate, lambda z, x, j: (z ^ 1, x, j))
        lent = permute(lent, lambda z, x, j: (z, x, j ^ 2))
        mixed = project(inner, deliver(0, 0), passed, weights, mate_weights, [lent])
        return permute(mixed, lambda z, x, j: (z ^ ((j & 1) * 2 | (j >> 1)), x, z))

    in_specs = (P("tok", "feat"), P("tok", "feat"), P("tok", "feat"), P("feat", "tok"), P())
    return jax.shard_map(
        shards, mesh=mesh, in_specs=in_specs, out_specs=P("tok", "feat"), check_vma=False
    )
```

```python
import math
from functools import partial

import jax
import jax.numpy as jnp
import numpy as np
from jax import lax
from jax.experimental import pallas as pl
from jax.experimental.pallas import tpu as pltpu
from jax.sharding import PartitionSpec as P


HD = 128
ROPE_BASE = 500000.0
NEG_FILL = -1e30
LONGEST = (5, 8)
KERNEL_BYTES = 16 << 20
FAR_BLOCKS = 7


def locate(token_index, doc_lengths):
    doc_ends = jnp.cumsum(doc_lengths)
    starts = doc_ends - doc_lengths
    doc_ids = jnp.sum((token_index[:, None] >= doc_ends[None, :]).astype(jnp.int32), axis=1)
    number = jnp.arange(doc_lengths.shape[0], dtype=jnp.int32)
    first_token = jnp.sum(
        jnp.where(doc_ids[:, None] == number[None, :], starts[None, :], 0), axis=1
    )
    return (doc_ids, token_index - first_token)


def on_chip(*arrays):
    return [pltpu.with_memory_space_constraint(a, pltpu.VMEM) for a in arrays]


def sine_cosine(angle):
    turns = jnp.round(angle * (2.0 / math.pi))
    rest = ((angle - turns * 1.5703125) - turns * 4.837512969970703125e-4) - turns * 7.54978995489188216e-8
    square = rest * rest
    sine = (-1.9515295891e-4 * square + 8.3321608736e-3) * square - 1.6666654611e-1
    sine = sine * square * rest + rest
    cosine = (2.443315711809948e-5 * square - 1.388731625493765e-3) * square
    cosine = (cosine + 4.166664568298827e-2) * square * square - 0.5 * square + 1.0
    quarter = turns.astype(jnp.int32)
    swapped = (quarter & 1) == 1
    flip_sine = (quarter & 2) == 2
    flip_cosine = ((quarter + 1) & 2) == 2
    out_sine = jnp.where(swapped, cosine, sine)
    out_cosine = jnp.where(swapped, sine, cosine)
    return (
        jnp.where(flip_sine, -out_sine, out_sine),
        jnp.where(flip_cosine, -out_cosine, out_cosine),
    )


def doc_start(index, lengths_ref):
    start, end = jnp.zeros_like(index), jnp.int32(0)
    for n in range(lengths_ref.shape[0]):
        start = jnp.where(index >= end, end, start)
        end = end + lengths_ref[n]
    return start


def turn(block, cosine, sine):
    block = block.astype(jnp.float32)
    return (block * cosine + pltpu.roll(block, HD // 2, 1) * sine).astype(jnp.bfloat16)


def prepare_kernel(lengths_ref, freq_ref, q_ref, k_ref, *refs, reach):
    cos_ref, sin_ref, query_ref, key_ref = refs
    rows = k_ref.shape[0]
    first = lax.axis_index("tok") * rows
    lane = lax.broadcasted_iota(jnp.int32, (rows, HD), 1)
    sub = lax.broadcasted_iota(jnp.int32, (rows, HD), 0)
    freq = freq_ref[...]
    for n in range(reach + 1):
        index = first - (reach - n) * rows + sub
        start = doc_start(index, lengths_ref)
        sine, cosine = sine_cosine((index - start).astype(jnp.float32) * freq)
        sine = jnp.where(lane < HD // 2, -sine, sine)
        if n < reach:
            cos_ref[n * rows : (n + 1) * rows, :] = cosine
            sin_ref[n * rows : (n + 1) * rows, :] = sine
    for source, target in ((q_ref, query_ref), (k_ref, key_ref)):
        for h in range(source.shape[1] // HD):
            at = slice(h * HD, (h + 1) * HD)
            target[:, at] = turn(source[:, at], cosine, sine)


def attention_kernel(lengths_ref, cos_ref, sin_ref, q_ref, k_ref, v_ref, *refs, reach, relayed):
    out_ref, score_ref, weight_ref = refs[-3:]
    me = lax.axis_index("tok")
    far, taken = [], 0
    for targets in relayed:
        far.append(refs[taken][...])
        taken += 1
        if targets:
            here = me == targets[0]
            for t in targets[1:]:
                here = here | (me == t)
            far[-1] = jnp.where(here, far[-1], refs[taken][...])
            taken += 1
    rows = k_ref.shape[0]
    kv_heads = k_ref.shape[1] // HD
    group = q_ref.shape[1] // k_ref.shape[1]
    count = reach + 1
    first = lax.axis_index("tok") * rows
    scale = HD**-0.5 * math.log2(math.e)
    key_lane = lax.broadcasted_iota(jnp.int32, (rows, rows), 1)
    key_sub = lax.broadcasted_iota(jnp.int32, (rows, rows), 0)
    starts = doc_start(first + key_sub, lengths_ref)
    seen = [first - (reach - n) * rows + key_lane >= starts for n in range(count)]
    seen[reach] = seen[reach] & (key_lane <= key_sub)
    for g in range(kv_heads):
        at = slice(g * HD, (g + 1) * HD)
        at_v = slice((kv_heads + g) * HD, (kv_heads + g + 1) * HD)
        keys = []
        for n in range(reach):
            part = slice(n * rows, (n + 1) * rows)
            keys.append(turn(far[reach - n - 1][:, at], cos_ref[part, :], sin_ref[part, :]))
        keys = jnp.concatenate(keys + [k_ref[:, at]], axis=0)
        vals = jnp.concatenate(
            [far[reach - n - 1][:, at_v] for n in range(reach)] + [v_ref[:, at]], axis=0
        )
        query = jnp.concatenate(
            [q_ref[:, h * HD : (h + 1) * HD] for h in range(g * group, (g + 1) * group)], axis=0
        )
        score_ref[g] = lax.dot_general(
            query, keys, (((1,), (1,)), ((), ())), preferred_element_type=jnp.float32
        )
        totals = []
        for h in range(group):
            band = slice(h * rows, (h + 1) * rows)
            masked = [
                jnp.where(seen[n], score_ref[g, band, n * rows : (n + 1) * rows] * scale, NEG_FILL)
                for n in range(count)
            ]
            top = masked[0]
            for m in masked[1:]:
                top = jnp.maximum(top, m)
            top = jnp.max(top, axis=1, keepdims=True)
            total = None
            for n in range(count):
                w = jnp.exp2(masked[n] - top)
                total = w if total is None else total + w
                weight_ref[g, band, n * rows : (n + 1) * rows] = w.astype(jnp.bfloat16)
            totals.append(jnp.sum(total, axis=1, keepdims=True))
        update = jnp.dot(weight_ref[g], vals, preferred_element_type=jnp.float32)
        for h in range(group):
            piece = update[h * rows : (h + 1) * rows, :] / totals[h]
            head = g * group + h
            out_ref[:, head * HD : (head + 1) * HD] = piece.astype(jnp.bfloat16)


def attend_near(queries, keys, values, doc_lengths, reach, n_tok, inner):
    rows = queries.shape[0]
    kv_heads = keys.shape[1] // HD
    group = queries.shape[1] // keys.shape[1]
    both = jnp.concatenate([keys, values], axis=1)
    far = []
    base = n_tok // 2

    def shift(array, d, pairs):
        return lax.ppermute(array, "tok", [(i, i + d) for i in pairs])

    held = shift(both, base, range(n_tok - base))
    relayed = []
    for d in range(1, reach + 1):
        relayed.append([])
        if d == base:
            far.append(held)
            continue
        pairs = range(n_tok - d)
        if d > base or (d - base) % inner == 0:
            across = [i for i in pairs if i // base != (i + d) // base]
            relayed[-1] = [i + d for i in across if (i + base) // inner != (i + d) // inner]
        if relayed[-1]:
            far.append(shift(held, d - base, [t - d + base for t in relayed[-1]]))
        direct = [i for i in pairs if i + d not in relayed[-1]]
        if direct:
            far.append(shift(both, d, direct))
    half = np.arange(HD, dtype=np.float32) % (HD // 2)
    freq = jnp.asarray((ROPE_BASE ** (-(half * 2.0 / HD))).astype(np.float32).reshape(1, HD))
    vmem = pl.BlockSpec(memory_space=pltpu.VMEM)
    smem = pl.BlockSpec(memory_space=pltpu.SMEM)
    span = (reach + 1) * rows
    whole = pltpu.VMEM(queries.shape, jnp.bfloat16)
    settings = pltpu.CompilerParams(vmem_limit_bytes=KERNEL_BYTES)
    cosine, sine, query, key = pl.pallas_call(
        partial(prepare_kernel, reach=reach),
        out_shape=(
            pltpu.VMEM((reach * rows, HD), jnp.float32),
            pltpu.VMEM((reach * rows, HD), jnp.float32),
            whole,
            pltpu.VMEM(keys.shape, jnp.bfloat16),
        ),
        in_specs=[smem] + [vmem] * 3,
        out_specs=(vmem,) * 4,
        compiler_params=settings,
        name="prepare",
    )(doc_lengths, freq, *on_chip(queries, keys))
    return pl.pallas_call(
        partial(attention_kernel, reach=reach, relayed=relayed),
        out_shape=whole,
        in_specs=[smem] + [vmem] * (5 + len(far)),
        out_specs=vmem,
        scratch_shapes=[
            pltpu.VMEM((kv_heads, group * rows, span), jnp.float32),
            pltpu.VMEM((kv_heads, group * rows, span), jnp.bfloat16),
        ],
        compiler_params=settings,
        name="attention",
    )(doc_lengths, *on_chip(cosine, sine, query, key, values, *far))


def rotary(tensor, positions):
    half_size = tensor.shape[-1] // 2
    frequency = ROPE_BASE ** (-(jnp.arange(half_size, dtype=jnp.float32) * 2.0 / tensor.shape[-1]))
    angles = positions.astype(jnp.float32)[:, None] * frequency[None, :]
    cosine = jnp.cos(angles)[:, None, :]
    sine_part = jnp.sin(angles)[:, None, :]
    a = tensor[..., :half_size]
    b = tensor[..., half_size:]
    return jnp.concatenate([a * cosine - b * sine_part, b * cosine + a * sine_part], axis=-1)


def attend_far(queries, keys, values, doc_lengths):
    rows = queries.shape[0]
    heads, kv_heads = queries.shape[1] // HD, keys.shape[1] // HD
    own = lax.axis_index("tok") * rows + jnp.arange(rows, dtype=jnp.int32)
    docs, positions = locate(own, doc_lengths)
    rotated_q = rotary(queries.astype(jnp.float32).reshape(rows, heads, HD), positions)
    rotated_q = rotated_q.astype(jnp.bfloat16).reshape(rows, kv_heads, heads // kv_heads, HD)
    rotated_k = rotary(keys.astype(jnp.float32).reshape(rows, kv_heads, HD), positions)
    rotated_k = rotated_k.astype(jnp.bfloat16).reshape(rows, kv_heads * HD)
    all_k = lax.all_gather(rotated_k, "tok", axis=0, tiled=True)
    all_v = lax.all_gather(values, "tok", axis=0, tiled=True)
    step = 4 * rows

    def one_block(number, state):
        running, totals, weighted = state
        begin = number * step
        key = lax.dynamic_slice_in_dim(all_k, begin, step, 0).reshape(step, kv_heads, HD)
        value = lax.dynamic_slice_in_dim(all_v, begin, step, 0).reshape(step, kv_heads, HD)
        index = begin + jnp.arange(step, dtype=jnp.int32)
        key_docs, _ = locate(index, doc_lengths)
        scores = HD**-0.5 * jnp.einsum(
            "qgjd,kgd->gjqk", rotated_q, key, preferred_element_type=jnp.float32
        )
        visible = (docs[:, None] == key_docs[None, :]) & (index[None, :] <= own[:, None])
        scores = jnp.where(visible, scores, NEG_FILL)
        top = jnp.maximum(running, jnp.max(scores, axis=-1))
        factor = jnp.exp(running - top)
        weights = jnp.where(visible, jnp.exp(scores - top[..., None]), 0.0)
        totals = totals * factor + jnp.sum(weights, axis=-1)
        update = jnp.einsum(
            "gjqk,kgd->gjqd",
            weights.astype(jnp.bfloat16),
            value,
            preferred_element_type=jnp.float32,
        )
        return (top, totals, weighted * factor[..., None] + update)

    shape = (kv_heads, heads // kv_heads, rows)
    state = (
        jnp.full(shape, NEG_FILL, jnp.float32),
        jnp.zeros(shape, jnp.float32),
        jnp.zeros(shape + (HD,), jnp.float32),
    )
    _, totals, weighted = lax.fori_loop(0, all_k.shape[0] // step, one_block, state)
    output = (weighted / totals[..., None]).transpose(2, 0, 1, 3)
    return output.reshape(rows, heads * HD).astype(jnp.bfloat16)


def project_kernel(own_ref, mate_ref, *refs, inner, sides, added):
    weights, (*before, out_ref) = refs[: 2 * sides], refs[2 * sides :]
    pieces = []
    for n, (own_w, mate_w) in enumerate(zip(weights[:sides], weights[sides:])):
        own = jnp.dot(own_ref[...], own_w[...], preferred_element_type=jnp.float32)
        mate = jnp.dot(mate_ref[...], mate_w[...], preferred_element_type=jnp.float32)
        own, mate = (p.astype(jnp.bfloat16).astype(jnp.float32) for p in (own, mate))
        piece = own + mate
        if added:
            piece = piece + before[n][...].astype(jnp.float32)
        pieces.append(piece)
    straight = jnp.concatenate(pieces, axis=1)
    if sides > 1:
        flip = lax.rem(lax.axis_index("tok"), inner)
        straight = jnp.where(flip == 0, straight, jnp.concatenate(pieces[::-1], axis=1))
    out_ref[...] = straight.astype(jnp.bfloat16)


def project(inner, own, mate, own_weights, mate_weights, before):
    vmem = pl.BlockSpec(memory_space=pltpu.VMEM)
    operands = on_chip(own, mate, *own_weights, *mate_weights, *before)
    return pl.pallas_call(
        partial(project_kernel, inner=inner, sides=len(own_weights), added=len(before)),
        out_shape=pltpu.VMEM((own.shape[0], sum(w.shape[1] for w in own_weights)), jnp.bfloat16),
        in_specs=[vmem] * len(operands),
        out_specs=vmem,
        compiler_params=pltpu.CompilerParams(vmem_limit_bytes=KERNEL_BYTES),
    )(*operands)


def solution(mesh):
    n_tok, n_feat = mesh.shape["tok"], mesh.shape["feat"]
    inner = n_tok // n_feat

    def everyone(move):
        pairs = []
        for z in range(n_feat):
            for x in range(inner):
                for j in range(n_feat):
                    to_z, to_x, to_j = move(z, x, j)
                    pairs.append(
                        (
                            (z * inner + x) * n_feat + j,
                            (to_z * inner + to_x) * n_feat + to_j,
                        )
                    )
        return pairs

    def permute(array, move):
        return lax.ppermute(array, ("tok", "feat"), everyone(move))

    def shards(queries, keys, values, out_weight, doc_lengths):
        rows = queries.shape[0]
        longest = n_tok * rows * LONGEST[0] // LONGEST[1]
        reach = min(n_tok - 1, -(-(longest - 1) // rows))
        if reach <= FAR_BLOCKS:
            attended = attend_near(queries, keys, values, doc_lengths, reach, n_tok, inner)
        else:
            attended = attend_far(queries, keys, values, doc_lengths)
        if inner == 2:
            weights = [out_weight, permute(out_weight, lambda z, x, j: (z, 1 - x, j))]
        else:
            groups = [[z * inner + x for x in range(inner)] for z in range(n_feat)]
            weights = [
                lax.all_gather(
                    out_weight, "tok", axis=1, tiled=True, axis_index_groups=groups
                )
            ]
        mate_weights = []
        for w in weights:
            mate_weights.append(permute(w, lambda z, x, j: (z, x, j ^ 1)))

        def deliver(k, cross):
            def move(z, x, j):
                core = (j & 1) ^ cross
                return (z ^ (core * 2 | ((j >> 1) ^ k)), x, (j & 2) | core)

            return permute(attended, move)

        own, mate = deliver(1, 0), deliver(1, 1)
        lent = [project(inner, own, mate, [w], [m], []) for w, m in zip(weights, mate_weights)]
        passed = permute(mate, lambda z, x, j: (z ^ 1, x, j))
        for n, part in enumerate(lent):
            lent[n] = permute(part, lambda z, x, j: (z, x, j ^ 2))
        mixed = project(inner, deliver(0, 0), passed, weights, mate_weights, lent)
        return permute(mixed, lambda z, x, j: (z ^ ((j & 1) * 2 | (j >> 1)), x, z))

    in_specs = (P("tok", "feat"), P("tok", "feat"), P("tok", "feat"), P("feat", "tok"), P())
    return jax.shard_map(
        shards, mesh=mesh, in_specs=in_specs, out_specs=P("tok", "feat"), check_vma=False
    )
```
